1024 devices in a mesh: dp: 32 (over y, z_hi, core), tensor: 32 (over z_lo, x).
Axes of the slice: x: 4, y: 8, z: 16 (z_hi: 2, z_lo: 8; z = z_hi * 8 + z_lo), core: 2. Of those that a mesh axis runs over, the one named last changes fastest.
Arguments:
- hidden_in: bfloat16 [4096, 8192], P('dp'), may hold values from -20 to 20
- norm_gain: bfloat16 [8192], replicated, may hold values from 0.25 to 1.75
- q_weight: bfloat16 [8192, 8192], P(None, 'tensor'), as said below
- q_grad: bfloat16 [4096, 8192], P('dp', 'tensor'), may hold values from -6 to 6
- q_main: float32 [8192, 8192], P('dp', 'tensor'), may hold values from -6 to 6
- weight_main_gradient: float32 [8192], P('tensor'), may hold values from -6 to 6
Outputs:
- hidden_state_gradient: bfloat16 [4096, 8192], P('dp', 'tensor')
- q_main_new: float32 [8192, 8192], P('dp', 'tensor')
- weight_main_updated: float32 [8192], P('tensor')
The draws below stay inside these ranges and needn't reach their ends.
Inputs may be any that keep to these rules, and one draw needn't show every extreme that they name: `q_weight`: entries of mean 0 and deviation about 8192 ** -0.5.
All inputs are finite; a program needn't handle non-finite values.
Results may differ from the reference program's by a relative error of at most 0.03.
Values may be sent and summed in bfloat16 or wider, within the bound.
No kernel may reach another device: no remote copies, remote signals or barrier semaphores. Data moves between devices by JAX's collectives and lax.ppermute only.
A program may use at most 64 MiB of HBM per device.

```python
import jax
import jax.numpy as jnp
from jax import lax

D = 8192
TOK_DEV = 128
TOKENS = 4096
N_DP = 32
N_TENSOR = 32


def query_grads(key):
    grad_key = jax.random.fold_in(key, 11)
    values = jnp.clip(jax.random.normal(grad_key, (TOKENS, D), jnp.float32), -6.0, 6.0)
    return values.astype(jnp.bfloat16)


def query_weights(key):
    weight_key = jax.random.fold_in(key, 12)
    values = jnp.clip(jax.random.normal(weight_key, (D, D), jnp.float32), -6.0, 6.0) * D ** (-0.5)
    return values.astype(jnp.bfloat16)


def draw_q_grad(key, part):
    return query_grads(key)


def draw_q_weight(key, part):
    return query_weights(key)


def draw_hidden_in(key, part):
    grads = query_grads(key)
    weights = query_weights(key)
    direction = jnp.dot(grads, weights.T, preferred_element_type=jnp.float32)
    direction = direction * jax.lax.rsqrt(jnp.mean(direction * direction, axis=1, keepdims=True) + 1e-06)
    noise_key = jax.random.fold_in(key, 21)
    sign_key = jax.random.fold_in(key, 22)
    strength_key = jax.random.fold_in(key, 23)
    perm_key = jax.random.fold_in(key, 24)
    noise = jnp.clip(jax.random.normal(noise_key, (TOKENS, D), jnp.float32), -6.0, 6.0)
    owners = jax.random.permutation(perm_key, N_DP)
    row_block = jnp.arange(TOKENS, dtype=jnp.int32) // TOK_DEV
    col_block = jnp.arange(D, dtype=jnp.int32) // (D // N_DP)
    spike = jnp.where(owners[row_block][:, None] == col_block[None, :], 2.5, 1.0)
    signs = jnp.where(jax.random.bernoulli(sign_key, 0.5, (TOKENS, 1)), 1.0, -1.0)
    strength = jax.random.uniform(strength_key, (TOKENS, 1), jnp.float32, 0.6, 1.2)
    values = noise * spike + signs * strength * direction
    return jnp.clip(values, -20.0, 20.0).astype(jnp.bfloat16)


def level_of(stream_key, dims, shards, low, largest):
    factor_of = 1.0
    for axis_at, shards_of in shards:
        draws = jax.random.uniform(jax.random.fold_in(jax.random.fold_in(stream_key, 6), axis_at), (shards_of,), jnp.float32, low / len(shards), largest / len(shards))
        factor_of = factor_of * jnp.repeat(jnp.exp(draws), dims[axis_at] // shards_of).reshape((-1,) + (1,) * (len(dims) - 1 - axis_at))
    return factor_of


def centred(rng, dims, width, reach, split=(), kind=jnp.bfloat16):
    gain = level_of(rng, dims, split, -0.22, 0.18) if split else 1.0
    values = jax.random.normal(rng, dims, jnp.float32) * width * gain
    return jnp.minimum(jnp.maximum(values, -reach), reach).astype(kind)


def setup_inputs(seed: int = 0) -> dict:
    arg_keys = jax.random.split(jax.random.key(seed), 7)
    hidden_in = draw_hidden_in(jax.random.fold_in(arg_keys[6], 71), 0)
    norm_gain = jnp.clip(1.0 + 0.15 * jax.random.normal(arg_keys[1], (D,), jnp.float32), 0.25, 1.75).astype(jnp.bfloat16)
    q_weight = draw_q_weight(jax.random.fold_in(arg_keys[6], 71), 0)
    q_grad = draw_q_grad(jax.random.fold_in(arg_keys[6], 71), 0)
    q_main = centred(arg_keys[4], (D, D), 1.0, 6.0, ((0, 32), (1, 32)), jnp.float32)
    weight_main_gradient = centred(arg_keys[5], (D,), 1.0, 6.0, ((0, 32),), jnp.float32)
    return {"hidden_in": hidden_in, "norm_gain": norm_gain, "q_weight": q_weight, "q_grad": q_grad, "q_main": q_main, "weight_main_gradient": weight_main_gradient}


def reference(hidden_in, norm_gain, q_weight, q_grad, q_main, weight_main_gradient):
    hidden_state = hidden_in.astype(jnp.float32)
    inverse_root_mean = lax.rsqrt(lax.optimization_barrier(jnp.mean(hidden_state * hidden_state, axis=-1, keepdims=True)) + 1e-05)
    normalized_rows = hidden_state * inverse_root_mean
    norm_weight = norm_gain.astype(jnp.float32)
    normalized_input = (normalized_rows * norm_weight).astype(jnp.bfloat16)
    block = D // N_TENSOR

    def tensor_step(total, index):
        start = (index * block).astype(jnp.int32)
        grad_cols = lax.dynamic_slice_in_dim(q_grad, start, block, 1)
        weight_cols = lax.dynamic_slice_in_dim(q_weight, start, block, 1)
        term = jnp.dot(grad_cols, weight_cols.T, preferred_element_type=jnp.float32).astype(jnp.bfloat16)
        term = lax.optimization_barrier(term)
        return (total + term.astype(jnp.float32), None)
    normalized_gradient, unused = lax.scan(tensor_step, jnp.zeros((TOKENS, D), jnp.float32), jnp.arange(N_TENSOR, dtype=jnp.int32))
    scaled_gradient = normalized_gradient * norm_weight
    row_statistic = lax.optimization_barrier(jnp.mean(scaled_gradient * normalized_rows, axis=-1, keepdims=True))
    hidden_state_gradient = (inverse_root_mean * (scaled_gradient - normalized_rows * row_statistic)).astype(jnp.bfloat16)
    weight_main_updated = weight_main_gradient + lax.optimization_barrier(jnp.sum(normalized_gradient * normalized_rows, axis=0)) / N_DP

    def data_step(total, index):
        start = (index * TOK_DEV).astype(jnp.int32)
        rows = lax.dynamic_slice_in_dim(normalized_input, start, TOK_DEV, 0)
        grads = lax.dynamic_slice_in_dim(q_grad, start, TOK_DEV, 0)
        term = (jnp.dot(rows.T, grads, preferred_element_type=jnp.float32) / N_DP).astype(jnp.bfloat16)
        term = lax.optimization_barrier(term)
        return (total + term.astype(jnp.float32), None)
    q_main_new, unused_two = lax.scan(data_step, q_main, jnp.arange(N_DP, dtype=jnp.int32))
    return (hidden_state_gradient, q_main_new, weight_main_updated)
```

```python
import functools

import jax
import jax.numpy as jnp
from jax import lax
from jax.experimental import pallas as pl
from jax.experimental.pallas import tpu as pltpu
from jax.sharding import Mesh, PartitionSpec as P


BF = jnp.bfloat16
F32 = jnp.float32
NY, NH, NC, NZ, NX = 8, 2, 2, 8, 4
TOK = 128
D = 8192
B = 256
VM = pl.BlockSpec(memory_space=pltpu.VMEM)


def cost(flops, nbytes):
    return pl.CostEstimate(flops=flops, bytes_accessed=nbytes, transcendentals=0)


def norm_kernel(sc, h_ref, g_ref, q_ref, send_ref, own_ref, rinv_ref):
    par, core = sc[0], sc[1]

    def rows(r, _):
        at = pl.ds(pl.multiple_of(r * 16, 16), 16)
        acc = jnp.zeros((16, 128), F32)
        for j in range(D // 128):
            h = h_ref[at, j * 128 : (j + 1) * 128].astype(F32)
            acc = acc + h * h
        mean = jnp.sum(acc, axis=1, keepdims=True) / D
        rinv_ref[at, :] = lax.rsqrt(mean + 1e-05)
        return 0

    lax.fori_loop(0, TOK // 16, rows, 0)
    rinv = rinv_ref[...]

    def place(out, which):
        def one(j, _):
            o, k, zh = j // 8, (j // 2) % 4, j % 2
            y = 2 * k + jnp.where(o == 0, 1 - par, par)
            src = pl.multiple_of((y * 4 + zh * 2 + which) * B, B)
            dst = pl.multiple_of(j * B, B)
            h = h_ref[:, pl.ds(src, B)].astype(F32)
            g = g_ref[:, pl.ds(src, B)].astype(F32)
            out[:, pl.ds(dst, B)] = (h * rinv * g).astype(BF)
            return 0

        lax.fori_loop(0, 16, one, 0)

    place(send_ref, 1 - core)
    send_ref[:, 16 * B :] = q_ref[...]
    place(own_ref, core)


def norm(sc, hidden, gain, q_grad):
    return pl.pallas_call(
        norm_kernel,
        out_shape=(
            jax.ShapeDtypeStruct((TOK, 17 * B), BF),
            jax.ShapeDtypeStruct((TOK, 16 * B), BF),
            jax.ShapeDtypeStruct((TOK, 1), F32),
        ),
        in_specs=[pl.BlockSpec(memory_space=pltpu.SMEM), VM, VM, VM],
        out_specs=(VM, VM, VM),
        cost_estimate=cost(6 * TOK * D, 4 * TOK * D),
        name="norm",
    )(sc, hidden, gain, q_grad)


def eye():
    a = lax.broadcasted_iota(jnp.int32, (128, 128), 0)
    b = lax.broadcasted_iota(jnp.int32, (128, 128), 1)
    return a == b


def stat_rows(row):
    hi = row.astype(BF).astype(F32)
    lo = row - hi
    both = jnp.concatenate([hi, lo], axis=1)
    first = lax.broadcasted_iota(jnp.int32, (8, 256), 0) == 0
    return jnp.where(first, jnp.broadcast_to(both, (8, 256)), 0.0).astype(BF)


def stat_of(block):
    both = jnp.sum(block.astype(F32), axis=0, keepdims=True)
    return both[:, :128] + both[:, 128:]


def partial_kernel(q_ref, w_ref, h_ref, g_ref, rinv_ref, out_ref, acc_ref):
    z = pl.program_id(0)

    @pl.when(z == 0)
    def _():
        acc_ref[...] = jnp.zeros_like(acc_ref)

    q = q_ref[...]
    for x in range(NX):
        at = slice(x * B, (x + 1) * B)
        p = lax.dot_general(q, w_ref[at, :], (((1,), (1,)), ((), ())), preferred_element_type=F32)
        p = p.astype(BF)
        out_ref[x, pl.ds(pl.multiple_of(z * TOK, TOK), TOK), :] = p
        t = p.astype(F32) * (h_ref[:, at].astype(F32) * g_ref[:, at].astype(F32))
        acc_ref[...] += t[:, :128] + t[:, 128:]

    @pl.when(z == NZ - 1)
    def _():
        s = jnp.sum(acc_ref[...], axis=1, keepdims=True) * rinv_ref[...]
        row = jnp.sum(jnp.where(eye(), s, 0.0), axis=0, keepdims=True)
        rows = stat_rows(row)
        for x in range(NX):
            out_ref[x, NZ * TOK :, :] = rows


def partial(q_grad, weight, hidden, gain, rinv):
    w = NX * B
    return pl.pallas_call(
        partial_kernel,
        grid=(NZ,),
        out_shape=jax.ShapeDtypeStruct((NX, NZ * TOK + 8, B), BF),
        in_specs=[
            pl.BlockSpec((TOK, B), lambda z: (0, 0)),
            pl.BlockSpec((w, B), lambda z: (z, 0)),
            pl.BlockSpec((TOK, w), lambda z: (0, z)),
            pl.BlockSpec((1, w), lambda z: (0, z)),
            pl.BlockSpec((TOK, 1), lambda z: (0, 0)),
        ],
        out_specs=pl.BlockSpec((NX, NZ * TOK + 8, B), lambda z: (0, 0, 0)),
        scratch_shapes=[pltpu.VMEM((TOK, 128), F32)],
        cost_estimate=cost(2 * TOK * D * B, 8 * 2**20),
        name="partial",
    )(q_grad, weight, hidden, gain, rinv)


def sum_x_kernel(sc, in_ref, send_ref, keep_ref):
    par = sc[0]

    def total(at):
        s = in_ref[0, at, :].astype(F32)
        for x in range(1, NX):
            s = s + in_ref[x, at, :].astype(F32)
        return s

    for k in range(4):
        at = pl.ds(pl.multiple_of((2 * k + 1 - par) * TOK, TOK), TOK)
        send_ref[k * TOK : (k + 1) * TOK, :] = total(at).astype(BF)
        at = pl.ds(pl.multiple_of((2 * k + par) * TOK, TOK), TOK)
        keep_ref[k * TOK : (k + 1) * TOK, :] = total(at).astype(BF)
    rows = stat_rows(stat_of(total(slice(NZ * TOK, NZ * TOK + 8))))
    send_ref[4 * TOK :, :] = rows
    keep_ref[4 * TOK :, :] = rows


def sum_x(sc, got):
    shape = jax.ShapeDtypeStruct((4 * TOK + 8, B), BF)
    return pl.pallas_call(
        sum_x_kernel,
        out_shape=(shape, shape),
        in_specs=[pl.BlockSpec(memory_space=pltpu.SMEM), VM],
        out_specs=(VM, VM),
        cost_estimate=cost(TOK * D, 3 * 2**20),
        name="sum_x",
    )(sc, got)


def sum_pair_kernel(keep_ref, got_ref, out_ref):
    for k in range(4):
        at = slice(k * TOK, (k + 1) * TOK)
        s = keep_ref[at, :].astype(F32) + got_ref[at, :].astype(F32)
        out_ref[k, :TOK, :] = s.astype(BF)
    at = slice(4 * TOK, 4 * TOK + 8)
    rows = stat_rows(stat_of(keep_ref[at, :].astype(F32) + got_ref[at, :].astype(F32)))
    for k in range(4):
        out_ref[k, TOK:, :] = rows


def sum_pair(keep, got):
    return pl.pallas_call(
        sum_pair_kernel,
        out_shape=jax.ShapeDtypeStruct((4, TOK + 8, B), BF),
        in_specs=[VM, VM],
        out_specs=VM,
        cost_estimate=cost(TOK * D // 4, 2**20),
        name="sum_pair",
    )(keep, got)


def finish_kernel(sc, got_ref, h_ref, g_ref, rinv_ref, out_ref, gain_ref):
    grad = got_ref[0, :TOK, :].astype(F32)
    stat = stat_of(got_ref[0, TOK:, :])
    for k in range(1, 4):
        grad = grad + got_ref[k, :TOK, :].astype(F32)
        stat = stat + stat_of(got_ref[k, TOK:, :])
    stat = jnp.sum(jnp.where(eye(), stat, 0.0), axis=1, keepdims=True) / D
    rinv = rinv_ref[...]
    xhat = h_ref[...].astype(F32) * rinv
    out_ref[...] = (rinv * (grad * g_ref[...].astype(F32) - xhat * stat)).astype(BF)
    gain_ref[...] = jnp.sum(grad * xhat, axis=0, keepdims=True)


def finish(sc, got, hidden, gain, rinv):
    spec = pltpu.PrefetchScalarGridSpec(
        num_scalar_prefetch=1,
        grid=(1,),
        in_specs=[
            pl.BlockSpec((4, TOK + 8, B), lambda i, s: (0, 0, 0)),
            pl.BlockSpec((TOK, B), lambda i, s: (0, s[0])),
            pl.BlockSpec((1, B), lambda i, s: (0, s[0])),
            pl.BlockSpec((TOK, 1), lambda i, s: (0, 0)),
        ],
        out_specs=(
            pl.BlockSpec((TOK, B), lambda i, s: (0, 0)),
            pl.BlockSpec((1, B), lambda i, s: (0, 0)),
        ),
    )
    return pl.pallas_call(
        finish_kernel,
        grid_spec=spec,
        out_shape=(jax.ShapeDtypeStruct((TOK, B), BF), jax.ShapeDtypeStruct((1, B), F32)),
        cost_estimate=cost(TOK * B * 16, 2**20),
        name="finish",
    )(sc, got, hidden, gain, rinv)


def product_kernel(own_ref, got_ref, q_ref, gq_ref, left_ref, right_ref, keep_ref):
    i = pl.program_id(0)
    a = jnp.concatenate([own_ref[...], got_ref[...]], axis=0)
    q = jnp.concatenate([q_ref[...], gq_ref[...]], axis=0)
    p = lax.dot_general(a, q, (((0,), (0,)), ((), ())), preferred_element_type=F32).astype(BF)

    @pl.when(i < 4)
    def _():
        left_ref[...] = p[:, :128]
        right_ref[...] = p[:, 128:]

    @pl.when(i >= 4)
    def _():
        keep_ref[...] = p


def product(own, got, q_grad):
    w = 2 * B
    half = jax.ShapeDtypeStruct((4 * w, 128), BF)
    first = lambda i: (jnp.minimum(i, 3), 0)
    return pl.pallas_call(
        product_kernel,
        grid=(8,),
        out_shape=(half, half, jax.ShapeDtypeStruct((4 * w, B), BF)),
        in_specs=[
            pl.BlockSpec((TOK, w), lambda i: (0, i)),
            pl.BlockSpec((TOK, w), lambda i: (0, i)),
            pl.BlockSpec((TOK, B), lambda i: (0, 0)),
            pl.BlockSpec((TOK, B), lambda i: (0, 16)),
        ],
        out_specs=(
            pl.BlockSpec((w, 128), first),
            pl.BlockSpec((w, 128), first),
            pl.BlockSpec((w, B), lambda i: (jnp.maximum(i - 4, 0), 0)),
        ),
        cost_estimate=cost(2 * TOK * D * B, 4 * 2**20),
        name="product",
    )(own, got, q_grad, got)


def sum_y_kernel(sc, keep_ref, left_ref, right_ref, o0, o1, o2, o3):
    k = sc[0]
    for r, out in enumerate((o0, o1, o2, o3)):
        at = pl.ds(pl.multiple_of(lax.rem(k + r, 4) * 512, 512), 512)
        out[:, :128] = (keep_ref[at, :128].astype(F32) + left_ref[at, :].astype(F32)).astype(BF)
        out[:, 128:] = (keep_ref[at, 128:].astype(F32) + right_ref[at, :].astype(F32)).astype(BF)


def sum_y(sc, keep, left, right):
    shape = jax.ShapeDtypeStruct((512, B), BF)
    return pl.pallas_call(
        sum_y_kernel,
        out_shape=(shape,) * 4,
        in_specs=[pl.BlockSpec(memory_space=pltpu.SMEM), VM, VM, VM],
        out_specs=(VM,) * 4,
        cost_estimate=cost(TOK * D, 3 * 2**20),
        name="sum_y",
    )(sc, keep, left, right)


def sum_y4_kernel(sc, a, b, c, d, send_ref, keep_ref):
    zh = sc[0]

    def total(z):
        at = pl.ds(pl.multiple_of(z * B, B), B)
        return a[at, :].astype(F32) + b[at, :].astype(F32) + c[at, :].astype(F32) + d[at, :].astype(F32)

    send_ref[...] = total(1 - zh).astype(BF)
    keep_ref[...] = total(zh)


def sum_y4(sc, parts):
    return pl.pallas_call(
        sum_y4_kernel,
        out_shape=(jax.ShapeDtypeStruct((B, B), BF), jax.ShapeDtypeStruct((B, B), F32)),
        in_specs=[pl.BlockSpec(memory_space=pltpu.SMEM), VM, VM, VM, VM],
        out_specs=(VM, VM),
        cost_estimate=cost(TOK * D, 3 * 2**20),
        name="sum_y4",
    )(sc, *parts)


def pairs(n, f):
    return [(i, f(i) % n) for i in range(n)]


def body(hidden, gain, weight, q_grad, q_main, gain_main):
    y, zh, c = lax.axis_index("y"), lax.axis_index("zh"), lax.axis_index("c")
    zl, x = lax.axis_index("zl"), lax.axis_index("x")
    ints = lambda *v: jnp.stack([jnp.asarray(i, jnp.int32) for i in v])
    gain2 = gain.reshape(1, D)

    send, own, rinv = norm(ints(y % 2, c), hidden, gain2, q_grad)
    got = lax.ppermute(send, "c", [(0, 1), (1, 0)])
    part = partial(q_grad, weight, hidden, gain2, rinv)
    part = lax.all_to_all(part, "x", 0, 0, tiled=True)

    left, right, keep = product(own, got, q_grad)
    left = lax.ppermute(left, "y", pairs(NY, lambda i: i ^ 1))
    right = lax.ppermute(right, "y", pairs(NY, lambda i: i + 1 if i % 2 else i - 1))

    send_z, keep_z = sum_x(ints(zl % 2), part)
    got_z = lax.ppermute(send_z, "zl", pairs(NZ, lambda i: i ^ 1))

    p0, p1, p2, p3 = sum_y(ints(y // 2), keep, left, right)
    p2 = lax.ppermute(p2, "y", pairs(NY, lambda i: i + 4))
    p1 = lax.ppermute(p1, "y", pairs(NY, lambda i: i + 2))
    p3 = lax.ppermute(p3, "y", pairs(NY, lambda i: i + 6))

    four = sum_pair(keep_z, got_z)
    evens, odds = [0, 2, 4, 6], [1, 3, 5, 7]
    four = lax.all_to_all(four, "zl", 0, 0, tiled=True, axis_index_groups=[evens, odds])

    send_h, keep_h = sum_y4(ints(zh), (p0, p1, p2, p3))
    got_h = lax.ppermute(send_h, "zh", [(0, 1), (1, 0)])

    grad, own_gain = finish(ints(zl * NX + x), four, hidden, gain2, rinv)
    dp = NY * NH * NC
    all_gain = lax.all_to_all(
        jnp.broadcast_to(own_gain[None], (dp, 1, B)), ("y", "zh", "c"), 0, 0, tiled=True
    )
    q_new = q_main + (keep_h + got_h.astype(F32)) / dp
    gain_new = gain_main + jnp.sum(all_gain, axis=(0, 1)) / dp
    return grad, q_new, gain_new


def solution(mesh):
    fine = Mesh(mesh.devices.reshape(NY, NH, NC, NZ, NX), ("y", "zh", "c", "zl", "x"))
    dp, tp = ("y", "zh", "c"), ("zl", "x")
    in_specs = (P(dp, None), P(), P(None, tp), P(dp, tp), P(dp, tp), P(tp))
    out_specs = (P(dp, tp), P(dp, tp), P(tp))
    return jax.shard_map(body, mesh=fine, in_specs=in_specs, out_specs=out_specs, check_vma=False)
```

```python
import functools

import jax
import jax.numpy as jnp
from jax import lax
from jax.experimental import pallas as pl
from jax.experimental.pallas import tpu as pltpu
from jax.sharding import Mesh, PartitionSpec as P


BF = jnp.bfloat16
F32 = jnp.float32
NY, NH, NC, NZ, NX = 8, 2, 2, 8, 4
TOK = 128
D = 8192
B = 256
MB = 2**20
VM = pl.BlockSpec(memory_space=pltpu.VMEM)


def cost(flops, nbytes):
    return pl.CostEstimate(flops=flops, bytes_accessed=nbytes, transcendentals=0)


def params(mib):
    return pltpu.CompilerParams(vmem_limit_bytes=mib * MB)


def call(kernel, out_shape, args, mib, flops, nbytes, **kw):
    return pl.pallas_call(
        kernel,
        out_shape=out_shape,
        compiler_params=params(mib),
        cost_estimate=cost(flops, nbytes),
        **kw,
    )(*args)


def aligned(start, size):
    return pl.ds(pl.multiple_of(start, size), size)


def two_rows(g_ref, block):
    at = lambda i: g_ref[pl.ds(2 * block + i, 1), :]
    return jnp.concatenate([at(0), at(1)], axis=1)


ROWS = 64


def norm_kernel(h_ref, g_ref, q_ref, send_ref, own_ref, rinv_ref, g32):
    par, core = lax.rem(lax.axis_index("y"), 2), lax.axis_index("c")
    g32[...] = g_ref[...].astype(F32)
    acc = jnp.zeros((ROWS, 128), F32)
    for j in range(D // 128):
        h = h_ref[:, j * 128 : (j + 1) * 128].astype(F32)
        acc = acc + h * h
    rinv = lax.rsqrt(jnp.sum(acc, axis=1, keepdims=True) / D + 1e-05)
    rinv_ref[...] = rinv
    for out, which in ((send_ref, 1 - core), (own_ref, core)):
        for j in range(16):
            o, k, zh = j // 8, (j // 2) % 4, j % 2
            y = 2 * k + (1 - par if o == 0 else par)
            block = y * 4 + zh * 2 + which
            h = h_ref[:, aligned(block * B, B)].astype(F32)
            out[:, j * B : (j + 1) * B] = (h * rinv * two_rows(g32, block)).astype(BF)
    send_ref[:, 16 * B :] = q_ref[...]


def norm(hidden, gain, q_grad):
    row = lambda n: pl.BlockSpec((ROWS, n), lambda i: (i, 0))
    return call(
        norm_kernel,
        (
            jax.ShapeDtypeStruct((TOK, 17 * B), BF),
            jax.ShapeDtypeStruct((TOK, 16 * B), BF),
            jax.ShapeDtypeStruct((TOK, 1), F32),
        ),
        (hidden, gain, q_grad),
        16,
        6 * TOK * D,
        4 * TOK * D,
        grid=(TOK // ROWS,),
        in_specs=[row(D), pl.BlockSpec((64, 128), lambda i: (0, 0)), row(B)],
        out_specs=(row(17 * B), row(16 * B), row(1)),
        scratch_shapes=[pltpu.VMEM((64, 128), F32)],
        name="norm",
    )


def eye():
    a = lax.broadcasted_iota(jnp.int32, (128, 128), 0)
    b = lax.broadcasted_iota(jnp.int32, (128, 128), 1)
    return a == b


def stat_rows(row):
    hi = row.astype(BF).astype(F32)
    both = jnp.concatenate([hi, row - hi], axis=1)
    first = lax.broadcasted_iota(jnp.int32, (8, 256), 0) == 0
    return jnp.where(first, jnp.broadcast_to(both, (8, 256)), 0.0).astype(BF)


def stat_of(block):
    both = jnp.sum(block.astype(F32), axis=0, keepdims=True)
    return both[:, :128] + both[:, 128:]


def partial_kernel(q_ref, w_ref, h_ref, g_ref, rinv_ref, out_ref):
    q = q_ref[...]
    g = g_ref[...].astype(F32)
    acc = jnp.zeros((TOK, 128), F32)
    for z in range(NZ):
        for x in range(NX):
            b = z * NX + x
            at = slice(b * B, (b + 1) * B)
            p = lax.dot_general(q, w_ref[at, :], (((1,), (1,)), ((), ())), preferred_element_type=F32)
            p = p.astype(BF)
            out_ref[x, z * TOK : (z + 1) * TOK, :] = p
            t = p.astype(F32) * h_ref[:, at].astype(F32)
            acc = acc + t[:, :128] * g[2 * b : 2 * b + 1, :] + t[:, 128:] * g[2 * b + 1 : 2 * b + 2, :]
    s = jnp.sum(acc, axis=1, keepdims=True) * rinv_ref[...]
    rows = stat_rows(jnp.sum(jnp.where(eye(), s, 0.0), axis=0, keepdims=True))
    for x in range(NX):
        out_ref[x, NZ * TOK :, :] = rows


def partial(q_grad, weight, hidden, gain, rinv):
    return call(
        partial_kernel,
        jax.ShapeDtypeStruct((NX, NZ * TOK + 8, B), BF),
        (q_grad, weight, hidden, gain, rinv),
        24,
        2 * TOK * D * B,
        8 * MB,
        in_specs=[VM] * 5,
        out_specs=VM,
        name="partial",
    )


def sum_x_kernel(in_ref, send_ref, keep_ref):
    bit = lax.rem(lax.axis_index("zl"), 2)

    def total(at):
        s = in_ref[0, at, :].astype(F32)
        for x in range(1, NX):
            s = s + in_ref[x, at, :].astype(F32)
        return s

    for k in range(4):
        at = slice(k * TOK, (k + 1) * TOK)
        send_ref[at, :] = total(aligned((2 * k + 1 - bit) * TOK, TOK)).astype(BF)
    rows = stat_rows(stat_of(total(slice(NZ * TOK, NZ * TOK + 8))))
    send_ref[4 * TOK :, :] = rows
    for k in range(4):
        at = slice(k * TOK, (k + 1) * TOK)
        keep_ref[at, :] = total(aligned((2 * k + bit) * TOK, TOK))
    keep_ref[4 * TOK :, :] = rows.astype(F32)


def sum_x(got):
    rows = 4 * TOK + 8
    return call(
        sum_x_kernel,
        (jax.ShapeDtypeStruct((rows, B), BF), jax.ShapeDtypeStruct((rows, B), F32)),
        (got,),
        12,
        TOK * D,
        4 * MB,
        in_specs=[VM],
        out_specs=(VM, VM),
        name="sum_x",
    )


def sum_z_kernel(count, shift, keep_ref, got_ref, send_ref, out_ref):
    bit = lax.rem(lax.div(lax.axis_index("zl"), shift), 2)
    half = count // 2

    def total(at):
        return keep_ref[at, :] + got_ref[at, :].astype(F32)

    for k in range(half):
        at = slice(k * TOK, (k + 1) * TOK)
        send_ref[at, :] = total(aligned((2 * k + 1 - bit) * TOK, TOK)).astype(BF)
    rows = stat_rows(stat_of(total(slice(count * TOK, count * TOK + 8))))
    send_ref[half * TOK :, :] = rows
    for k in range(half):
        at = slice(k * TOK, (k + 1) * TOK)
        out_ref[at, :] = total(aligned((2 * k + bit) * TOK, TOK))
    out_ref[half * TOK :, :] = rows.astype(F32)


def sum_z(keep, got, count, shift):
    rows = count // 2 * TOK + 8
    return call(
        functools.partial(sum_z_kernel, count, shift),
        (jax.ShapeDtypeStruct((rows, B), BF), jax.ShapeDtypeStruct((rows, B), F32)),
        (keep, got),
        6,
        count * TOK * B,
        count * MB // 2,
        in_specs=[VM, VM],
        out_specs=(VM, VM),
        name=f"sum_z{shift}",
    )


def finish_kernel(keep_ref, got_ref, h_ref, g_ref, rinv_ref, out_ref, gain_ref, g32):
    own = lax.axis_index("zl") * NX + lax.axis_index("x")
    g32[...] = g_ref[...].astype(F32)
    grad = keep_ref[:TOK, :] + got_ref[:TOK, :].astype(F32)
    stat = stat_of(keep_ref[TOK:, :] + got_ref[TOK:, :].astype(F32))
    stat = jnp.sum(jnp.where(eye(), stat, 0.0), axis=1, keepdims=True) / D
    rinv = rinv_ref[...]
    xhat = h_ref[:, aligned(own * B, B)].astype(F32) * rinv
    total = jnp.sum(grad * xhat, axis=0, keepdims=True)
    for i in range(NY * NH * NC):
        gain_ref[i] = total
    out_ref[...] = (rinv * (grad * two_rows(g32, own) - xhat * stat)).astype(BF)


def finish(keep, got, hidden, gain, rinv):
    return call(
        finish_kernel,
        (
            jax.ShapeDtypeStruct((TOK, B), BF),
            jax.ShapeDtypeStruct((NY * NH * NC, 1, B), F32),
        ),
        (keep, got, hidden, gain, rinv),
        10,
        TOK * B * 16,
        MB,
        in_specs=[VM] * 5,
        out_specs=(VM, VM),
        scratch_shapes=[pltpu.VMEM((64, 128), F32)],
        name="finish",
    )


STEPS = 4


def product_kernel(own_ref, got_ref, q_ref, gq_ref, left_ref, right_ref, keep_ref):
    i = pl.program_id(0)
    a = jnp.concatenate([own_ref[...], got_ref[...]], axis=0)
    q = jnp.concatenate([q_ref[...], gq_ref[...]], axis=0)
    p = lax.dot_general(q, a, (((0,), (0,)), ((), ())), preferred_element_type=F32).astype(BF)

    @pl.when(i < STEPS // 2)
    def _():
        left_ref[...] = p[:128, :]
        right_ref[...] = p[128:, :]

    @pl.when(i >= STEPS // 2)
    def _():
        keep_ref[...] = p


def product(own, got, q_grad):
    w = 16 * B // STEPS
    half = jax.ShapeDtypeStruct((128, 8 * B), BF)
    first = lambda i: (0, jnp.minimum(i, STEPS // 2 - 1))
    return call(
        product_kernel,
        (half, half, jax.ShapeDtypeStruct((B, 8 * B), BF)),
        (own, got, q_grad, got),
        16,
        2 * TOK * D * B,
        4 * MB,
        grid=(STEPS,),
        in_specs=[
            pl.BlockSpec((TOK, w), lambda i: (0, i)),
            pl.BlockSpec((TOK, w), lambda i: (0, i)),
            pl.BlockSpec((TOK, B), lambda i: (0, 0)),
            pl.BlockSpec((TOK, B), lambda i: (0, 16)),
        ],
        out_specs=(
            pl.BlockSpec((128, w), first),
            pl.BlockSpec((128, w), first),
            pl.BlockSpec((B, w), lambda i: (0, jnp.maximum(i - STEPS // 2, 0))),
        ),
        name="product",
    )


def sum_y_kernel(keep_ref, left_ref, right_ref, out_ref):
    for k in range(4):
        at = slice(k * 512, (k + 1) * 512)
        out_ref[k, :128, :] = (keep_ref[:128, at].astype(F32) + left_ref[:, at].astype(F32)).astype(BF)
        out_ref[k, 128:, :] = (keep_ref[128:, at].astype(F32) + right_ref[:, at].astype(F32)).astype(BF)


def sum_y(keep, left, right):
    return call(
        sum_y_kernel,
        jax.ShapeDtypeStruct((4, B, 512), BF),
        (keep, left, right),
        8,
        TOK * D,
        3 * MB,
        in_specs=[VM] * 3,
        out_specs=VM,
        name="sum_y",
    )


def sum_y4_kernel(in_ref, send_ref, keep_ref):
    zh = lax.axis_index("zh")

    def total(z):
        at = aligned(z * B, B)
        s = in_ref[0, :, at].astype(F32)
        for k in range(1, 4):
            s = s + in_ref[k, :, at].astype(F32)
        return s

    send_ref[...] = total(1 - zh).astype(BF)
    keep_ref[...] = total(zh)


def sum_y4(got):
    return call(
        sum_y4_kernel,
        (jax.ShapeDtypeStruct((B, B), BF), jax.ShapeDtypeStruct((B, B), F32)),
        (got,),
        6,
        TOK * D,
        2 * MB,
        in_specs=[VM],
        out_specs=(VM, VM),
        name="sum_y4",
    )


def last_kernel(main_ref, keep_ref, got_ref, out_ref):
    s = keep_ref[...] + got_ref[...].astype(F32)
    out_ref[...] = main_ref[...] + s.T / (NY * NH * NC)


def last(main, keep, got):
    return call(
        last_kernel,
        jax.ShapeDtypeStruct((B, B), F32),
        (main, keep, got),
        4,
        B * B * 4,
        MB,
        in_specs=[VM] * 3,
        out_specs=VM,
        name="last",
    )


def pairs(n, f):
    return [(i, f(i) % n) for i in range(n)]


def swap(v, axis, n, f):
    return lax.ppermute(v, axis, pairs(n, f))


def exchange(v, axis, **kw):
    return lax.all_to_all(v, axis, 0, 0, tiled=True, **kw)


def body(hidden, gain, weight, q_grad, q_main, gain_main):
    gain2 = gain.reshape(64, 128)
    send, own, rinv = norm(hidden, gain2, q_grad)
    got = swap(send, "c", NC, lambda i: i ^ 1)
    part = partial(q_grad, weight, hidden, gain2, rinv)
    part = exchange(part, "x")

    left, right, keep = product(own, got, q_grad)
    left = swap(left, "y", NY, lambda i: i ^ 1)
    right = swap(right, "y", NY, lambda i: i + 1 if i % 2 else i - 1)

    send1, keep1 = sum_x(part)
    got1 = swap(send1, "zl", NZ, lambda i: i ^ 1)

    four = sum_y(keep, left, right)
    four = exchange(four, "y", axis_index_groups=[[0, 2, 4, 6], [1, 3, 5, 7]])

    send2, keep2 = sum_z(keep1, got1, 4, 2)
    got2 = swap(send2, "zl", NZ, lambda i: i ^ 2)
    send3, keep3 = sum_z(keep2, got2, 2, 4)
    got3 = swap(send3, "zl", NZ, lambda i: i ^ 4)
    grad, all_gain = finish(keep3, got3, hidden, gain2, rinv)
    all_gain = exchange(all_gain, ("y", "zh", "c"))

    send_h, keep_h = sum_y4(four)
    got_h = swap(send_h, "zh", NH, lambda i: i ^ 1)
    q_new = last(q_main, keep_h, got_h)
    gain_new = gain_main + jnp.sum(all_gain, axis=(0, 1)) / (NY * NH * NC)
    return grad, q_new, gain_new


def solution(mesh):
    fine = Mesh(mesh.devices.reshape(NY, NH, NC, NZ, NX), ("y", "zh", "c", "zl", "x"))
    dp, tp = ("y", "zh", "c"), ("zl", "x")
    in_specs = (P(dp, None), P(), P(None, tp), P(dp, tp), P(dp, tp), P(tp))
    out_specs = (P(dp, tp), P(dp, tp), P(tp))
    return jax.shard_map(body, mesh=fine, in_specs=in_specs, out_specs=out_specs, check_vma=False)
```

```python
import functools

import jax
import jax.numpy as jnp
from jax import lax
from jax.experimental import pallas as pl
from jax.experimental.pallas import tpu as pltpu
from jax.sharding import Mesh, PartitionSpec as P


BF = jnp.bfloat16
F32 = jnp.float32
NY, NH, NC, NZ, NX = 8, 2, 2, 8, 4
TOK = 128
D = 8192
B = 256
MB = 2**20
VM = pl.BlockSpec(memory_space=pltpu.VMEM)


def cost(flops, nbytes):
    return pl.CostEstimate(flops=flops, bytes_accessed=nbytes, transcendentals=0)


def params(mib):
    return pltpu.CompilerParams(vmem_limit_bytes=mib * MB if mib else None)


def call(kernel, out_shape, args, mib, flops, nbytes, **kw):
    return pl.pallas_call(
        kernel,
        out_shape=out_shape,
        compiler_params=params(mib),
        cost_estimate=cost(flops, nbytes),
        **kw,
    )(*args)


def aligned(start, size):
    return pl.ds(pl.multiple_of(start, size), size)


def two_rows(g_ref, block):
    at = lambda i: g_ref[pl.ds(2 * block + i, 1), :]
    return jnp.concatenate([at(0), at(1)], axis=1)


ROWS = 64


def norm_kernel(h_ref, g_ref, q_ref, send_ref, own_ref, rinv_ref, g32):
    par, core = lax.rem(lax.axis_index("y"), 2), lax.axis_index("c")
    g32[...] = g_ref[...].astype(F32)
    acc = jnp.zeros((ROWS, 128), F32)
    for j in range(D // 128):
        h = h_ref[:, j * 128 : (j + 1) * 128].astype(F32)
        acc = acc + h * h
    rinv = lax.rsqrt(jnp.sum(acc, axis=1, keepdims=True) / D + 1e-05)
    rinv_ref[...] = rinv
    for out, which in ((send_ref, 1 - core), (own_ref, core)):
        for j in range(16):
            o, k, zh = j // 8, (j // 2) % 4, j % 2
            y = 2 * k + (1 - par if o == 0 else par)
            block = y * 4 + zh * 2 + which
            h = h_ref[:, aligned(block * B, B)].astype(F32)
            out[:, j * B : (j + 1) * B] = (h * rinv * two_rows(g32, block)).astype(BF)
    send_ref[:, 16 * B :] = q_ref[...]


def norm(hidden, gain, q_grad):
    row = lambda n: pl.BlockSpec((ROWS, n), lambda i: (i, 0))
    return call(
        norm_kernel,
        (
            jax.ShapeDtypeStruct((TOK, 17 * B), BF),
            jax.ShapeDtypeStruct((TOK, 16 * B), BF),
            jax.ShapeDtypeStruct((TOK, 1), F32),
        ),
        (hidden, gain, q_grad),
        None,
        6 * TOK * D,
        4 * TOK * D,
        grid=(TOK // ROWS,),
        in_specs=[row(D), pl.BlockSpec((64, 128), lambda i: (0, 0)), row(B)],
        out_specs=(row(17 * B), row(16 * B), row(1)),
        scratch_shapes=[pltpu.VMEM((64, 128), F32)],
        name="norm",
    )


def eye():
    a = lax.broadcasted_iota(jnp.int32, (128, 128), 0)
    b = lax.broadcasted_iota(jnp.int32, (128, 128), 1)
    return a == b


def stat_rows(row):
    hi = row.astype(BF).astype(F32)
    both = jnp.concatenate([hi, row - hi], axis=1)
    first = lax.broadcasted_iota(jnp.int32, (8, 256), 0) == 0
    return jnp.where(first, jnp.broadcast_to(both, (8, 256)), 0.0).astype(BF)


def stat_of(block):
    both = jnp.sum(block.astype(F32), axis=0, keepdims=True)
    return both[:, :128] + both[:, 128:]


ZQ = NZ // 2
NG = 2 * NX
PIECE = ZQ * TOK + 8


def partial_kernel(q_ref, g_ref, w_hbm, h_hbm, out_hbm, w_ref, h_ref, out_ref, w_sem, h_sem, out_sem):
    wide = NX * B

    def w_copy(z):
        at = slice(z * wide, (z + 1) * wide)
        return pltpu.make_async_copy(w_hbm.at[at, :], w_ref.at[at, :], w_sem.at[z])

    def h_copy(z):
        at = slice(z * wide, (z + 1) * wide)
        return pltpu.make_async_copy(h_hbm.at[:, at], h_ref.at[:, at], h_sem.at[z])

    def out_copy(z, x):
        at = (z % 2 * NX + x, slice(z // 2 * TOK, (z // 2 + 1) * TOK))
        return pltpu.make_async_copy(out_ref.at[at], out_hbm.at[at], out_sem.at[z * NX + x])

    def stat_copy(d):
        at = (d, slice(ZQ * TOK, PIECE))
        return pltpu.make_async_copy(out_ref.at[at], out_hbm.at[at], out_sem.at[NZ * NX + d])

    for z in range(NZ):
        w_copy(z).start()
        h_copy(z).start()
    q = q_ref[...]
    g = g_ref[...].astype(F32)
    acc = jnp.zeros((TOK, 128), F32)
    for z in range(NZ):
        w_copy(z).wait()
        h_copy(z).wait()
        for x in range(NX):
            b = z * NX + x
            at = slice(b * B, (b + 1) * B)
            p = lax.dot_general(q, w_ref[at, :], (((1,), (1,)), ((), ())), preferred_element_type=F32)
            p = p.astype(BF)
            out_ref[z % 2 * NX + x, z // 2 * TOK : (z // 2 + 1) * TOK, :] = p
            t = p.astype(F32) * h_ref[:, at].astype(F32)
            acc = acc + t[:, :128] * g[2 * b : 2 * b + 1, :] + t[:, 128:] * g[2 * b + 1 : 2 * b + 2, :]
        if z > 0:
            for x in range(NX):
                out_copy(z - 1, x).start()
    s = jnp.sum(acc, axis=1, keepdims=True)
    rows = stat_rows(jnp.sum(jnp.where(eye(), s, 0.0), axis=0, keepdims=True))
    for d in range(NG):
        out_ref[d, ZQ * TOK :, :] = rows
    for x in range(NX):
        out_copy(NZ - 1, x).start()
    for d in range(NG):
        stat_copy(d).start()
    for z in range(NZ):
        for x in range(NX):
            out_copy(z, x).wait()
    for d in range(NG):
        stat_copy(d).wait()


HBM = pl.BlockSpec(memory_space=pltpu.HBM)


def partial(q_grad, weight, hidden, gain):
    return call(
        partial_kernel,
        jax.ShapeDtypeStruct((NG, PIECE, B), BF),
        (q_grad, gain, weight, hidden),
        None,
        2 * TOK * D * B,
        8 * MB,
        in_specs=[VM, VM, HBM, HBM],
        out_specs=HBM,
        scratch_shapes=[
            pltpu.VMEM((D, B), BF),
            pltpu.VMEM((TOK, D), BF),
            pltpu.VMEM((NG, PIECE, B), BF),
            pltpu.SemaphoreType.DMA((NZ,)),
            pltpu.SemaphoreType.DMA((NZ,)),
            pltpu.SemaphoreType.DMA((NZ * NX + NG,)),
        ],
        name="partial",
    )


def sum_xz_kernel(in_ref, send_ref, keep_ref):
    bit = lax.rem(lax.div(lax.axis_index("zl"), 2), 2)

    def total(at):
        s = in_ref[0, at, :].astype(F32)
        for d in range(1, NG):
            s = s + in_ref[d, at, :].astype(F32)
        return s

    rows = stat_rows(stat_of(total(slice(ZQ * TOK, PIECE))))
    for k in range(ZQ // 2):
        at = slice(k * TOK, (k + 1) * TOK)
        send_ref[at, :] = total(aligned((2 * k + 1 - bit) * TOK, TOK)).astype(BF)
        keep_ref[at, :] = total(aligned((2 * k + bit) * TOK, TOK))
    send_ref[ZQ // 2 * TOK :, :] = rows
    keep_ref[ZQ // 2 * TOK :, :] = rows.astype(F32)


def sum_xz(got):
    rows = ZQ // 2 * TOK + 8
    return call(
        sum_xz_kernel,
        (jax.ShapeDtypeStruct((rows, B), BF), jax.ShapeDtypeStruct((rows, B), F32)),
        (got,),
        12,
        TOK * D,
        4 * MB,
        in_specs=[VM],
        out_specs=(VM, VM),
        name="sum_xz",
    )


def sum_z_kernel(count, shift, keep_ref, got_ref, send_ref, out_ref):
    bit = lax.rem(lax.div(lax.axis_index("zl"), shift), 2)
    half = count // 2

    def total(at):
        return keep_ref[at, :] + got_ref[at, :].astype(F32)

    for k in range(half):
        at = slice(k * TOK, (k + 1) * TOK)
        send_ref[at, :] = total(aligned((2 * k + 1 - bit) * TOK, TOK)).astype(BF)
    rows = stat_rows(stat_of(total(slice(count * TOK, count * TOK + 8))))
    send_ref[half * TOK :, :] = rows
    for k in range(half):
        at = slice(k * TOK, (k + 1) * TOK)
        out_ref[at, :] = total(aligned((2 * k + bit) * TOK, TOK))
    out_ref[half * TOK :, :] = rows.astype(F32)


def sum_z(keep, got, count, shift):
    rows = count // 2 * TOK + 8
    return call(
        functools.partial(sum_z_kernel, count, shift),
        (jax.ShapeDtypeStruct((rows, B), BF), jax.ShapeDtypeStruct((rows, B), F32)),
        (keep, got),
        6,
        count * TOK * B,
        count * MB // 2,
        in_specs=[VM, VM],
        out_specs=(VM, VM),
        name=f"sum_z{shift}",
    )


def finish_kernel(keep_ref, got_ref, h_ref, g_ref, rinv_ref, out_ref, gain_ref, g32):
    own = lax.axis_index("zl") * NX + lax.axis_index("x")
    g32[...] = g_ref[...].astype(F32)
    grad = keep_ref[:TOK, :] + got_ref[:TOK, :].astype(F32)
    stat = stat_of(keep_ref[TOK:, :] + got_ref[TOK:, :].astype(F32))
    rinv = rinv_ref[...]
    stat = jnp.sum(jnp.where(eye(), stat, 0.0), axis=1, keepdims=True) * rinv / D
    xhat = h_ref[:, aligned(own * B, B)].astype(F32) * rinv
    total = jnp.sum(grad * xhat, axis=0, keepdims=True)
    for i in range(NY * NH * NC):
        gain_ref[i] = total
    out_ref[...] = (rinv * (grad * two_rows(g32, own) - xhat * stat)).astype(BF)


def finish(keep, got, hidden, gain, rinv):
    return call(
        finish_kernel,
        (
            jax.ShapeDtypeStruct((TOK, B), BF),
            jax.ShapeDtypeStruct((NY * NH * NC, 1, B), F32),
        ),
        (keep, got, hidden, gain, rinv),
        10,
        TOK * B * 16,
        MB,
        in_specs=[VM] * 5,
        out_specs=(VM, VM),
        scratch_shapes=[pltpu.VMEM((64, 128), F32)],
        name="finish",
    )


STEPS = 4


def product_kernel(own_ref, got_ref, q_ref, gq_ref, left_ref, right_ref, keep_ref):
    i = pl.program_id(0)
    a = jnp.concatenate([own_ref[...], got_ref[...]], axis=0)
    q = jnp.concatenate([q_ref[...], gq_ref[...]], axis=0)
    p = lax.dot_general(q, a, (((0,), (0,)), ((), ())), preferred_element_type=F32).astype(BF)

    @pl.when(i < STEPS // 2)
    def _():
        left_ref[...] = p[:128, :]
        right_ref[...] = p[128:, :]

    @pl.when(i >= STEPS // 2)
    def _():
        keep_ref[...] = p


def product(own, got, q_grad):
    w = 16 * B // STEPS
    half = jax.ShapeDtypeStruct((128, 8 * B), BF)
    first = lambda i: (0, jnp.minimum(i, STEPS // 2 - 1))
    return call(
        product_kernel,
        (half, half, jax.ShapeDtypeStruct((B, 8 * B), BF)),
        (own, got, q_grad, got),
        16,
        2 * TOK * D * B,
        4 * MB,
        grid=(STEPS,),
        in_specs=[
            pl.BlockSpec((TOK, w), lambda i: (0, i)),
            pl.BlockSpec((TOK, w), lambda i: (0, i)),
            pl.BlockSpec((TOK, B), lambda i: (0, 0)),
            pl.BlockSpec((TOK, B), lambda i: (0, 16)),
        ],
        out_specs=(
            pl.BlockSpec((128, w), first),
            pl.BlockSpec((128, w), first),
            pl.BlockSpec((B, w), lambda i: (0, jnp.maximum(i - STEPS // 2, 0))),
        ),
        name="product",
    )


def sum_y_kernel(keep_ref, left_ref, right_ref, out_ref):
    out_ref[0, :128, :] = (keep_ref[:128, :].astype(F32) + left_ref[...].astype(F32)).astype(BF)
    out_ref[0, 128:, :] = (keep_ref[128:, :].astype(F32) + right_ref[...].astype(F32)).astype(BF)


def sum_y(keep, left, right):
    return call(
        sum_y_kernel,
        jax.ShapeDtypeStruct((4, B, 512), BF),
        (keep, left, right),
        8,
        TOK * D,
        3 * MB,
        grid=(4,),
        in_specs=[
            pl.BlockSpec((B, 512), lambda k: (0, k)),
            pl.BlockSpec((128, 512), lambda k: (0, k)),
            pl.BlockSpec((128, 512), lambda k: (0, k)),
        ],
        out_specs=pl.BlockSpec((1, B, 512), lambda k: (k, 0, 0)),
        name="sum_y",
    )


def sum_y4_kernel(in_ref, send_ref, keep_ref):
    zh = lax.axis_index("zh")

    def total(z):
        at = aligned(z * B, B)
        s = in_ref[0, :, at].astype(F32)
        for k in range(1, 4):
            s = s + in_ref[k, :, at].astype(F32)
        return s

    send_ref[...] = total(1 - zh).astype(BF)
    keep_ref[...] = total(zh)


def sum_y4(got):
    return call(
        sum_y4_kernel,
        (jax.ShapeDtypeStruct((B, B), BF), jax.ShapeDtypeStruct((B, B), F32)),
        (got,),
        6,
        TOK * D,
        2 * MB,
        in_specs=[VM],
        out_specs=(VM, VM),
        name="sum_y4",
    )


def last_kernel(main_ref, keep_ref, got_ref, out_ref):
    s = keep_ref[...] + got_ref[...].astype(F32)
    out_ref[...] = main_ref[...] + s.T / (NY * NH * NC)


def last(main, keep, got):
    return call(
        last_kernel,
        jax.ShapeDtypeStruct((B, B), F32),
        (main, keep, got),
        4,
        B * B * 4,
        MB,
        in_specs=[VM] * 3,
        out_specs=VM,
        name="last",
    )


def pairs(n, f):
    return [(i, f(i) % n) for i in range(n)]


def swap(v, axis, n, f):
    return lax.ppermute(v, axis, pairs(n, f))


def exchange(v, axis, **kw):
    return lax.all_to_all(v, axis, 0, 0, tiled=True, **kw)


def body(hidden, gain, weight, q_grad, q_main, gain_main):
    gain2 = gain.reshape(64, 128)
    part = partial(q_grad, weight, hidden, gain2)
    groups = [list(range(i * NG, (i + 1) * NG)) for i in range(NZ * NX // NG)]
    part = exchange(part, ("zl", "x"), axis_index_groups=groups)

    send, own, rinv = norm(hidden, gain2, q_grad)
    got = swap(send, "c", NC, lambda i: i ^ 1)
    left, right, keep = product(own, got, q_grad)
    left = swap(left, "y", NY, lambda i: i ^ 1)
    right = swap(right, "y", NY, lambda i: i + 1 if i % 2 else i - 1)

    send2, keep2 = sum_xz(part)
    got2 = swap(send2, "zl", NZ, lambda i: i ^ 2)

    four = sum_y(keep, left, right)
    four = exchange(four, "y", axis_index_groups=[[0, 2, 4, 6], [1, 3, 5, 7]])

    send3, keep3 = sum_z(keep2, got2, 2, 4)
    got3 = swap(send3, "zl", NZ, lambda i: i ^ 4)
    grad, all_gain = finish(keep3, got3, hidden, gain2, rinv)
    all_gain = exchange(all_gain, ("y", "zh", "c"))

    send_h, keep_h = sum_y4(four)
    got_h = swap(send_h, "zh", NH, lambda i: i ^ 1)
    q_new = last(q_main, keep_h, got_h)
    gain_new = gain_main + jnp.sum(all_gain, axis=(0, 1)) / (NY * NH * NC)
    return grad, q_new, gain_new


def solution(mesh):
    fine = Mesh(mesh.devices.reshape(NY, NH, NC, NZ, NX), ("y", "zh", "c", "zl", "x"))
    dp, tp = ("y", "zh", "c"), ("zl", "x")
    in_specs = (P(dp, None), P(), P(None, tp), P(dp, tp), P(dp, tp), P(tp))
    out_specs = (P(dp, tp), P(dp, tp), P(tp))
    return jax.shard_map(body, mesh=fine, in_specs=in_specs, out_specs=out_specs, check_vma=False)
```

```python
import functools

import jax
import jax.numpy as jnp
from jax import lax
from jax.experimental import pallas as pl
from jax.experimental.pallas import tpu as pltpu
from jax.sharding import Mesh, PartitionSpec as P


BF = jnp.bfloat16
F32 = jnp.float32
NY, NH, NC, NZ, NX = 8, 2, 2, 8, 4
TOK = 128
D = 8192
B = 256
MB = 2**20
VM = pl.BlockSpec(memory_space=pltpu.VMEM)


def cost(flops, nbytes):
    return pl.CostEstimate(flops=flops, bytes_accessed=nbytes, transcendentals=0)


def params(mib):
    return pltpu.CompilerParams(vmem_limit_bytes=mib * MB if mib else None)


def call(kernel, out_shape, args, mib, flops, nbytes, **kw):
    return pl.pallas_call(
        kernel,
        out_shape=out_shape,
        compiler_params=params(mib),
        cost_estimate=cost(flops, nbytes),
        **kw,
    )(*args)


def aligned(start, size):
    return pl.ds(pl.multiple_of(start, size), size)


def two_rows(g_ref, block):
    at = lambda i: g_ref[pl.ds(2 * block + i, 1), :]
    return jnp.concatenate([at(0), at(1)], axis=1)


def eye():
    a = lax.broadcasted_iota(jnp.int32, (128, 128), 0)
    b = lax.broadcasted_iota(jnp.int32, (128, 128), 1)
    return a == b


def stat_rows(row):
    hi = row.astype(BF).astype(F32)
    both = jnp.concatenate([hi, row - hi], axis=1)
    first = lax.broadcasted_iota(jnp.int32, (8, 256), 0) == 0
    return jnp.where(first, jnp.broadcast_to(both, (8, 256)), 0.0).astype(BF)


def stat_of(block):
    both = jnp.sum(block.astype(F32), axis=0, keepdims=True)
    return both[:, :128] + both[:, 128:]


ZQ = NZ // 2
NG = 2 * NX
PIECE = ZQ * TOK + 8
ROWS = 64
HBM = pl.BlockSpec(memory_space=pltpu.HBM)


def front_kernel(
    q_ref, g_ref, w_hbm, h_hbm, part_hbm, send_hbm, own_hbm, rinv_ref,
    w_ref, h_ref, part_ref, send_ref, own_ref, g32, w_sem, h_sem, out_sem, normed_sem,
):
    wide = NX * B
    par, core = lax.rem(lax.axis_index("y"), 2), lax.axis_index("c")

    def w_copy(z):
        at = slice(z * wide, (z + 1) * wide)
        return pltpu.make_async_copy(w_hbm.at[at, :], w_ref.at[at, :], w_sem.at[z])

    def h_copy(r):
        at = slice(r * ROWS, (r + 1) * ROWS)
        return pltpu.make_async_copy(h_hbm.at[at, :], h_ref.at[at, :], h_sem.at[r])

    def out_copy(z, x):
        at = (z % 2 * NX + x, slice(z // 2 * TOK, (z // 2 + 1) * TOK))
        return pltpu.make_async_copy(part_ref.at[at], part_hbm.at[at], out_sem.at[z * NX + x])

    def stat_copy(d):
        at = (d, slice(ZQ * TOK, PIECE))
        return pltpu.make_async_copy(part_ref.at[at], part_hbm.at[at], out_sem.at[NZ * NX + d])

    send_copy = pltpu.make_async_copy(send_ref, send_hbm, normed_sem.at[0])
    own_copy = pltpu.make_async_copy(own_ref, own_hbm, normed_sem.at[1])

    for r in range(TOK // ROWS):
        h_copy(r).start()
    g32[...] = g_ref[...].astype(F32)
    send_ref[:, 16 * B :] = q_ref[...]
    for r in range(TOK // ROWS):
        h_copy(r).wait()
        if r == 0:
            for z in range(NZ // 2):
                w_copy(z).start()
        at = slice(r * ROWS, (r + 1) * ROWS)
        acc = jnp.zeros((ROWS, 128), F32)
        for j in range(D // 128):
            h = h_ref[at, j * 128 : (j + 1) * 128].astype(F32)
            acc = acc + h * h
        rinv = lax.rsqrt(jnp.sum(acc, axis=1, keepdims=True) / D + 1e-05)
        rinv_ref[at, :] = rinv
        for out, which in ((send_ref, 1 - core), (own_ref, core)):
            for j in range(16):
                o, k, zh = j // 8, (j // 2) % 4, j % 2
                y = 2 * k + (1 - par if o == 0 else par)
                block = y * 4 + zh * 2 + which
                h = h_ref[at, aligned(block * B, B)].astype(F32)
                out[at, j * B : (j + 1) * B] = (h * rinv * two_rows(g32, block)).astype(BF)

    q = q_ref[...]
    g = g32[...]
    acc = jnp.zeros((TOK, 128), F32)
    for z in range(NZ):
        if z < NZ // 2:
            w_copy(z + NZ // 2).start()
        w_copy(z).wait()
        for x in range(NX):
            b = z * NX + x
            at = slice(b * B, (b + 1) * B)
            p = lax.dot_general(q, w_ref[at, :], (((1,), (1,)), ((), ())), preferred_element_type=F32)
            p = p.astype(BF)
            part_ref[z % 2 * NX + x, z // 2 * TOK : (z // 2 + 1) * TOK, :] = p
            t = p.astype(F32) * h_ref[:, at].astype(F32)
            acc = acc + t[:, :128] * g[2 * b : 2 * b + 1, :] + t[:, 128:] * g[2 * b + 1 : 2 * b + 2, :]
        if z == 0:
            send_copy.start()
            own_copy.start()
        else:
            for x in range(NX):
                out_copy(z - 1, x).start()
    s = jnp.sum(acc, axis=1, keepdims=True)
    rows = stat_rows(jnp.sum(jnp.where(eye(), s, 0.0), axis=0, keepdims=True))
    for d in range(NG):
        part_ref[d, ZQ * TOK :, :] = rows
    for x in range(NX):
        out_copy(NZ - 1, x).start()
    for d in range(NG):
        stat_copy(d).start()
    send_copy.wait()
    own_copy.wait()
    for z in range(NZ):
        for x in range(NX):
            out_copy(z, x).wait()
    for d in range(NG):
        stat_copy(d).wait()


def front(q_grad, gain, weight, hidden):
    return call(
        front_kernel,
        (
            jax.ShapeDtypeStruct((NG, PIECE, B), BF),
            jax.ShapeDtypeStruct((TOK, 17 * B), BF),
            jax.ShapeDtypeStruct((TOK, 16 * B), BF),
            jax.ShapeDtypeStruct((TOK, 1), F32),
        ),
        (q_grad, gain, weight, hidden),
        None,
        2 * TOK * D * B,
        12 * MB,
        in_specs=[VM, VM, HBM, HBM],
        out_specs=(HBM, HBM, HBM, VM),
        scratch_shapes=[
            pltpu.VMEM((D, B), BF),
            pltpu.VMEM((TOK, D), BF),
            pltpu.VMEM((NG, PIECE, B), BF),
            pltpu.VMEM((TOK, 17 * B), BF),
            pltpu.VMEM((TOK, 16 * B), BF),
            pltpu.VMEM((64, 128), F32),
            pltpu.SemaphoreType.DMA((NZ,)),
            pltpu.SemaphoreType.DMA((TOK // ROWS,)),
            pltpu.SemaphoreType.DMA((NZ * NX + NG,)),
            pltpu.SemaphoreType.DMA((2,)),
        ],
        name="front",
    )


def sum_xz_kernel(in_ref, send_ref, keep_ref):
    bit = lax.rem(lax.div(lax.axis_index("zl"), 2), 2)

    def total(at):
        s = in_ref[0, at, :].astype(F32)
        for d in range(1, NG):
            s = s + in_ref[d, at, :].astype(F32)
        return s

    rows = stat_rows(stat_of(total(slice(ZQ * TOK, PIECE))))
    for k in range(ZQ // 2):
        at = slice(k * TOK, (k + 1) * TOK)
        send_ref[at, :] = total(aligned((2 * k + 1 - bit) * TOK, TOK)).astype(BF)
        keep_ref[at, :] = total(aligned((2 * k + bit) * TOK, TOK))
    send_ref[ZQ // 2 * TOK :, :] = rows
    keep_ref[ZQ // 2 * TOK :, :] = rows.astype(F32)


def sum_xz(got):
    rows = ZQ // 2 * TOK + 8
    return call(
        sum_xz_kernel,
        (jax.ShapeDtypeStruct((rows, B), BF), jax.ShapeDtypeStruct((rows, B), F32)),
        (got,),
        12,
        TOK * D,
        4 * MB,
        in_specs=[VM],
        out_specs=(VM, VM),
        name="sum_xz",
    )


def sum_z_kernel(count, shift, keep_ref, got_ref, send_ref, out_ref):
    bit = lax.rem(lax.div(lax.axis_index("zl"), shift), 2)
    half = count // 2

    def total(at):
        return keep_ref[at, :] + got_ref[at, :].astype(F32)

    for k in range(half):
        at = slice(k * TOK, (k + 1) * TOK)
        send_ref[at, :] = total(aligned((2 * k + 1 - bit) * TOK, TOK)).astype(BF)
    rows = stat_rows(stat_of(total(slice(count * TOK, count * TOK + 8))))
    send_ref[half * TOK :, :] = rows
    for k in range(half):
        at = slice(k * TOK, (k + 1) * TOK)
        out_ref[at, :] = total(aligned((2 * k + bit) * TOK, TOK))
    out_ref[half * TOK :, :] = rows.astype(F32)


def sum_z(keep, got, count, shift):
    rows = count // 2 * TOK + 8
    return call(
        functools.partial(sum_z_kernel, count, shift),
        (jax.ShapeDtypeStruct((rows, B), BF), jax.ShapeDtypeStruct((rows, B), F32)),
        (keep, got),
        6,
        count * TOK * B,
        count * MB // 2,
        in_specs=[VM, VM],
        out_specs=(VM, VM),
        name=f"sum_z{shift}",
    )


def finish_kernel(keep_ref, got_ref, h_ref, g_ref, rinv_ref, out_ref, gain_ref, g32):
    own = lax.axis_index("zl") * NX + lax.axis_index("x")
    g32[...] = g_ref[...].astype(F32)
    grad = keep_ref[:TOK, :] + got_ref[:TOK, :].astype(F32)
    stat = stat_of(keep_ref[TOK:, :] + got_ref[TOK:, :].astype(F32))
    rinv = rinv_ref[...]
    stat = jnp.sum(jnp.where(eye(), stat, 0.0), axis=1, keepdims=True) * rinv / D
    xhat = h_ref[:, aligned(own * B, B)].astype(F32) * rinv
    gain_ref[...] = jnp.sum(grad * xhat, axis=0, keepdims=True)
    out_ref[...] = (rinv * (grad * two_rows(g32, own) - xhat * stat)).astype(BF)


def finish(keep, got, hidden, gain, rinv):
    return call(
        finish_kernel,
        (
            jax.ShapeDtypeStruct((TOK, B), BF),
            jax.ShapeDtypeStruct((1, B), F32),
        ),
        (keep, got, hidden, gain, rinv),
        10,
        TOK * B * 16,
        MB,
        in_specs=[VM] * 5,
        out_specs=(VM, VM),
        scratch_shapes=[pltpu.VMEM((64, 128), F32)],
        name="finish",
    )


STEPS = 4


def product_kernel(own_ref, got_ref, q_ref, gq_ref, left_ref, right_ref, keep_ref):
    i = pl.program_id(0)
    a = jnp.concatenate([own_ref[...], got_ref[...]], axis=0)
    q = jnp.concatenate([q_ref[...], gq_ref[...]], axis=0)
    p = lax.dot_general(q, a, (((0,), (0,)), ((), ())), preferred_element_type=F32).astype(BF)

    @pl.when(i < STEPS // 2)
    def _():
        left_ref[...] = p[:128, :]
        right_ref[...] = p[128:, :]

    @pl.when(i >= STEPS // 2)
    def _():
        keep_ref[...] = p


def product(own, got, q_grad):
    w = 16 * B // STEPS
    half = jax.ShapeDtypeStruct((128, 8 * B), BF)
    first = lambda i: (0, jnp.minimum(i, STEPS // 2 - 1))
    return call(
        product_kernel,
        (half, half, jax.ShapeDtypeStruct((B, 8 * B), BF)),
        (own, got, q_grad, got),
        16,
        2 * TOK * D * B,
        4 * MB,
        grid=(STEPS,),
        in_specs=[
            pl.BlockSpec((TOK, w), lambda i: (0, i)),
            pl.BlockSpec((TOK, w), lambda i: (0, i)),
            pl.BlockSpec((TOK, B), lambda i: (0, 0)),
            pl.BlockSpec((TOK, B), lambda i: (0, 16)),
        ],
        out_specs=(
            pl.BlockSpec((128, w), first),
            pl.BlockSpec((128, w), first),
            pl.BlockSpec((B, w), lambda i: (0, jnp.maximum(i - STEPS // 2, 0))),
        ),
        name="product",
    )


def sum_y_kernel(keep_ref, left_ref, right_ref, out_ref):
    for k in range(4):
        at = slice(k * 512, (k + 1) * 512)
        out_ref[k, :128, :] = (keep_ref[:128, at].astype(F32) + left_ref[:, at].astype(F32)).astype(BF)
        out_ref[k, 128:, :] = (keep_ref[128:, at].astype(F32) + right_ref[:, at].astype(F32)).astype(BF)


def sum_y(keep, left, right):
    return call(
        sum_y_kernel,
        jax.ShapeDtypeStruct((4, B, 512), BF),
        (keep, left, right),
        8,
        TOK * D,
        3 * MB,
        in_specs=[VM] * 3,
        out_specs=VM,
        name="sum_y",
    )


def sum_y4_kernel(in_ref, send_ref, keep_ref):
    zh = lax.axis_index("zh")

    def total(z):
        at = aligned(z * B, B)
        s = in_ref[0, :, at].astype(F32)
        for k in range(1, 4):
            s = s + in_ref[k, :, at].astype(F32)
        return s

    send_ref[...] = total(1 - zh).astype(BF)
    keep_ref[...] = total(zh)


def sum_y4(got):
    return call(
        sum_y4_kernel,
        (jax.ShapeDtypeStruct((B, B), BF), jax.ShapeDtypeStruct((B, B), F32)),
        (got,),
        6,
        TOK * D,
        2 * MB,
        in_specs=[VM],
        out_specs=(VM, VM),
        name="sum_y4",
    )


def last_kernel(main_ref, keep_ref, got_ref, out_ref):
    s = keep_ref[...] + got_ref[...].astype(F32)
    out_ref[...] = main_ref[...] + s.T / (NY * NH * NC)


def last(main, keep, got):
    return call(
        last_kernel,
        jax.ShapeDtypeStruct((B, B), F32),
        (main, keep, got),
        4,
        B * B * 4,
        MB,
        in_specs=[VM] * 3,
        out_specs=VM,
        name="last",
    )


def pairs(n, f):
    return [(i, f(i) % n) for i in range(n)]


def swap(v, axis, n, f):
    return lax.ppermute(v, axis, pairs(n, f))


def exchange(v, axis, **kw):
    return lax.all_to_all(v, axis, 0, 0, tiled=True, **kw)


def body(hidden, gain, weight, q_grad, q_main, gain_main):
    gain2 = gain.reshape(64, 128)
    part, send, own, rinv = front(q_grad, gain2, weight, hidden)
    got = swap(send, "c", NC, lambda i: i ^ 1)
    groups = [list(range(i * NG, (i + 1) * NG)) for i in range(NZ * NX // NG)]
    part = exchange(part, ("zl", "x"), axis_index_groups=groups)

    left, right, keep = product(own, got, q_grad)
    left = swap(left, "y", NY, lambda i: i ^ 1)
    right = swap(right, "y", NY, lambda i: i + 1 if i % 2 else i - 1)

    send2, keep2 = sum_xz(part)
    got2 = swap(send2, "zl", NZ, lambda i: i ^ 2)

    four = sum_y(keep, left, right)
    four = exchange(four, "y", axis_index_groups=[[0, 2, 4, 6], [1, 3, 5, 7]])

    send3, keep3 = sum_z(keep2, got2, 2, 4)
    got3 = swap(send3, "zl", NZ, lambda i: i ^ 4)
    grad, own_gain = finish(keep3, got3, hidden, gain2, rinv)
    got_gain = swap(own_gain, "zh", NH, lambda i: i ^ 1)

    send_h, keep_h = sum_y4(four)
    got_h = swap(send_h, "zh", NH, lambda i: i ^ 1)
    all_gain = jnp.broadcast_to((own_gain + got_gain)[None], (NY * NC, 1, B))
    all_gain = exchange(all_gain, ("y", "c"))
    q_new = last(q_main, keep_h, got_h)
    gain_new = gain_main + jnp.sum(all_gain, axis=(0, 1)) / (NY * NH * NC)
    return grad, q_new, gain_new


def solution(mesh):
    fine = Mesh(mesh.devices.reshape(NY, NH, NC, NZ, NX), ("y", "zh", "c", "zl", "x"))
    dp, tp = ("y", "zh", "c"), ("zl", "x")
    in_specs = (P(dp, None), P(), P(None, tp), P(dp, tp), P(dp, tp), P(tp))
    out_specs = (P(dp, tp), P(dp, tp), P(tp))
    return jax.shard_map(body, mesh=fine, in_specs=in_specs, out_specs=out_specs, check_vma=False)
```

```python
import functools

import jax
import jax.numpy as jnp
from jax import lax
from jax.experimental import pallas as pl
from jax.experimental.pallas import tpu as pltpu
from jax.sharding import Mesh, PartitionSpec as P


BF = jnp.bfloat16
F32 = jnp.float32
NY, NH, NC, NZ, NX = 8, 2, 2, 8, 4
TOK = 128
D = 8192
B = 256
MB = 2**20
VM = pl.BlockSpec(memory_space=pltpu.VMEM)


def cost(flops, nbytes):
    return pl.CostEstimate(flops=flops, bytes_accessed=nbytes, transcendentals=0)


def params(mib):
    return pltpu.CompilerParams(vmem_limit_bytes=mib * MB if mib else None)


def call(kernel, out_shape, args, mib, flops, nbytes, **kw):
    return pl.pallas_call(
        kernel,
        out_shape=out_shape,
        compiler_params=params(mib),
        cost_estimate=cost(flops, nbytes),
        **kw,
    )(*args)


def aligned(start, size):
    return pl.ds(pl.multiple_of(start, size), size)


def two_rows(g_ref, block):
    at = lambda i: g_ref[pl.ds(2 * block + i, 1), :]
    return jnp.concatenate([at(0), at(1)], axis=1)


ROWS = 64


def norm_kernel(h_ref, g_ref, q_ref, send_ref, own_ref, rinv_ref, g32):
    par, core = lax.rem(lax.axis_index("y"), 2), lax.axis_index("c")
    g32[...] = g_ref[...].astype(F32)
    acc = jnp.zeros((ROWS, 128), F32)
    for j in range(D // 128):
        h = h_ref[:, j * 128 : (j + 1) * 128].astype(F32)
        acc = acc + h * h
    rinv = lax.rsqrt(jnp.sum(acc, axis=1, keepdims=True) / D + 1e-05)
    rinv_ref[...] = rinv
    for out, which in ((send_ref, 1 - core), (own_ref, core)):
        for j in range(16):
            o, k, zh = j // 8, (j // 2) % 4, j % 2
            y = 2 * k + (1 - par if o == 0 else par)
            block = y * 4 + zh * 2 + which
            h = h_ref[:, aligned(block * B, B)].astype(F32)
            out[:, j * B : (j + 1) * B] = (h * rinv * two_rows(g32, block)).astype(BF)
    send_ref[:, 16 * B :] = q_ref[...]


def norm(hidden, gain, q_grad):
    row = lambda n: pl.BlockSpec((ROWS, n), lambda i: (i, 0))
    return call(
        norm_kernel,
        (
            jax.ShapeDtypeStruct((TOK, 17 * B), BF),
            jax.ShapeDtypeStruct((TOK, 16 * B), BF),
            jax.ShapeDtypeStruct((TOK, 1), F32),
        ),
        (hidden, gain, q_grad),
        None,
        6 * TOK * D,
        4 * TOK * D,
        grid=(TOK // ROWS,),
        in_specs=[row(D), pl.BlockSpec((64, 128), lambda i: (0, 0)), row(B)],
        out_specs=(row(17 * B), row(16 * B), row(1)),
        scratch_shapes=[pltpu.VMEM((64, 128), F32)],
        name="norm",
    )


def eye():
    a = lax.broadcasted_iota(jnp.int32, (128, 128), 0)
    b = lax.broadcasted_iota(jnp.int32, (128, 128), 1)
    return a == b


def stat_rows(row):
    hi = row.astype(BF).astype(F32)
    both = jnp.concatenate([hi, row - hi], axis=1)
    first = lax.broadcasted_iota(jnp.int32, (8, 256), 0) == 0
    return jnp.where(first, jnp.broadcast_to(both, (8, 256)), 0.0).astype(BF)


def stat_of(block):
    both = jnp.sum(block.astype(F32), axis=0, keepdims=True)
    return both[:, :128] + both[:, 128:]


ZQ = NZ // 2
NG = 2 * NX
PIECE = ZQ * TOK + 8
AHEAD = 2


def partial_kernel(q_ref, g_ref, w_hbm, h_hbm, out_hbm, w_ref, h_ref, out_ref, w_sem, h_sem, out_sem):
    wide = NX * B

    def w_copy(z):
        at = slice(z * wide, (z + 1) * wide)
        return pltpu.make_async_copy(w_hbm.at[at, :], w_ref.at[at, :], w_sem.at[z])

    def h_copy(z):
        at = slice(z * wide, (z + 1) * wide)
        return pltpu.make_async_copy(h_hbm.at[:, at], h_ref.at[:, at], h_sem.at[z])

    def out_copy(z, x):
        at = (z % 2 * NX + x, slice(z // 2 * TOK, (z // 2 + 1) * TOK))
        return pltpu.make_async_copy(out_ref.at[at], out_hbm.at[at], out_sem.at[z * NX + x])

    def stat_copy(d):
        at = (d, slice(ZQ * TOK, PIECE))
        return pltpu.make_async_copy(out_ref.at[at], out_hbm.at[at], out_sem.at[NZ * NX + d])

    for z in range(AHEAD):
        w_copy(z).start()
        h_copy(z).start()
    q = q_ref[...]
    g = g_ref[...].astype(F32)
    acc = jnp.zeros((TOK, 128), F32)
    for z in range(NZ):
        if z + AHEAD < NZ:
            w_copy(z + AHEAD).start()
            h_copy(z + AHEAD).start()
        w_copy(z).wait()
        h_copy(z).wait()
        for x in range(NX):
            b = z * NX + x
            at = slice(b * B, (b + 1) * B)
            p = lax.dot_general(q, w_ref[at, :], (((1,), (1,)), ((), ())), preferred_element_type=F32)
            p = p.astype(BF)
            out_ref[z % 2 * NX + x, z // 2 * TOK : (z // 2 + 1) * TOK, :] = p
            t = p.astype(F32) * h_ref[:, at].astype(F32)
            acc = acc + t[:, :128] * g[2 * b : 2 * b + 1, :] + t[:, 128:] * g[2 * b + 1 : 2 * b + 2, :]
        if z > 0:
            for x in range(NX):
                out_copy(z - 1, x).start()
    s = jnp.sum(acc, axis=1, keepdims=True)
    rows = stat_rows(jnp.sum(jnp.where(eye(), s, 0.0), axis=0, keepdims=True))
    for d in range(NG):
        out_ref[d, ZQ * TOK :, :] = rows
    for x in range(NX):
        out_copy(NZ - 1, x).start()
    for d in range(NG):
        stat_copy(d).start()
    for z in range(NZ):
        for x in range(NX):
            out_copy(z, x).wait()
    for d in range(NG):
        stat_copy(d).wait()


HBM = pl.BlockSpec(memory_space=pltpu.HBM)


def partial(q_grad, weight, hidden, gain):
    return call(
        partial_kernel,
        jax.ShapeDtypeStruct((NG, PIECE, B), BF),
        (q_grad, gain, weight, hidden),
        None,
        2 * TOK * D * B,
        8 * MB,
        in_specs=[VM, VM, HBM, HBM],
        out_specs=HBM,
        scratch_shapes=[
            pltpu.VMEM((D, B), BF),
            pltpu.VMEM((TOK, D), BF),
            pltpu.VMEM((NG, PIECE, B), BF),
            pltpu.SemaphoreType.DMA((NZ,)),
            pltpu.SemaphoreType.DMA((NZ,)),
            pltpu.SemaphoreType.DMA((NZ * NX + NG,)),
        ],
        name="partial",
    )


def sum_xz_kernel(in_ref, send_ref, keep_ref):
    bit = lax.rem(lax.div(lax.axis_index("zl"), 2), 2)

    def total(at):
        s = in_ref[0, at, :].astype(F32)
        for d in range(1, NG):
            s = s + in_ref[d, at, :].astype(F32)
        return s

    rows = stat_rows(stat_of(total(slice(ZQ * TOK, PIECE))))
    for k in range(ZQ // 2):
        at = slice(k * TOK, (k + 1) * TOK)
        send_ref[at, :] = total(aligned((2 * k + 1 - bit) * TOK, TOK)).astype(BF)
        keep_ref[at, :] = total(aligned((2 * k + bit) * TOK, TOK))
    send_ref[ZQ // 2 * TOK :, :] = rows
    keep_ref[ZQ // 2 * TOK :, :] = rows.astype(F32)


def sum_xz(got):
    rows = ZQ // 2 * TOK + 8
    return call(
        sum_xz_kernel,
        (jax.ShapeDtypeStruct((rows, B), BF), jax.ShapeDtypeStruct((rows, B), F32)),
        (got,),
        12,
        TOK * D,
        4 * MB,
        in_specs=[VM],
        out_specs=(VM, VM),
        name="sum_xz",
    )


def sum_z_kernel(count, shift, keep_ref, got_ref, send_ref, out_ref):
    bit = lax.rem(lax.div(lax.axis_index("zl"), shift), 2)
    half = count // 2

    def total(at):
        return keep_ref[at, :] + got_ref[at, :].astype(F32)

    for k in range(half):
        at = slice(k * TOK, (k + 1) * TOK)
        send_ref[at, :] = total(aligned((2 * k + 1 - bit) * TOK, TOK)).astype(BF)
    rows = stat_rows(stat_of(total(slice(count * TOK, count * TOK + 8))))
    send_ref[half * TOK :, :] = rows
    for k in range(half):
        at = slice(k * TOK, (k + 1) * TOK)
        out_ref[at, :] = total(aligned((2 * k + bit) * TOK, TOK))
    out_ref[half * TOK :, :] = rows.astype(F32)


def sum_z(keep, got, count, shift):
    rows = count // 2 * TOK + 8
    return call(
        functools.partial(sum_z_kernel, count, shift),
        (jax.ShapeDtypeStruct((rows, B), BF), jax.ShapeDtypeStruct((rows, B), F32)),
        (keep, got),
        6,
        count * TOK * B,
        count * MB // 2,
        in_specs=[VM, VM],
        out_specs=(VM, VM),
        name=f"sum_z{shift}",
    )


def finish_kernel(keep_ref, got_ref, h_ref, g_ref, rinv_ref, out_ref, gain_ref, g32):
    own = lax.axis_index("zl") * NX + lax.axis_index("x")
    g32[...] = g_ref[...].astype(F32)
    grad = keep_ref[:TOK, :] + got_ref[:TOK, :].astype(F32)
    stat = stat_of(keep_ref[TOK:, :] + got_ref[TOK:, :].astype(F32))
    rinv = rinv_ref[...]
    stat = jnp.sum(jnp.where(eye(), stat, 0.0), axis=1, keepdims=True) * rinv / D
    xhat = h_ref[:, aligned(own * B, B)].astype(F32) * rinv
    gain_ref[...] = jnp.sum(grad * xhat, axis=0, keepdims=True)
    out_ref[...] = (rinv * (grad * two_rows(g32, own) - xhat * stat)).astype(BF)


def finish(keep, got, hidden, gain, rinv):
    return call(
        finish_kernel,
        (
            jax.ShapeDtypeStruct((TOK, B), BF),
            jax.ShapeDtypeStruct((1, B), F32),
        ),
        (keep, got, hidden, gain, rinv),
        10,
        TOK * B * 16,
        MB,
        in_specs=[VM] * 5,
        out_specs=(VM, VM),
        scratch_shapes=[pltpu.VMEM((64, 128), F32)],
        name="finish",
    )


STEPS = 4


def product_kernel(own_ref, got_ref, q_ref, gq_ref, left_ref, right_ref, keep_ref):
    i = pl.program_id(0)
    a = jnp.concatenate([own_ref[...], got_ref[...]], axis=0)
    q = jnp.concatenate([q_ref[...], gq_ref[...]], axis=0)
    p = lax.dot_general(q, a, (((0,), (0,)), ((), ())), preferred_element_type=F32).astype(BF)

    @pl.when(i < STEPS // 2)
    def _():
        left_ref[...] = p[:128, :]
        right_ref[...] = p[128:, :]

    @pl.when(i >= STEPS // 2)
    def _():
        keep_ref[...] = p


def product(own, got, q_grad):
    w = 16 * B // STEPS
    half = jax.ShapeDtypeStruct((128, 8 * B), BF)
    first = lambda i: (0, jnp.minimum(i, STEPS // 2 - 1))
    return call(
        product_kernel,
        (half, half, jax.ShapeDtypeStruct((B, 8 * B), BF)),
        (own, got, q_grad, got),
        16,
        2 * TOK * D * B,
        4 * MB,
        grid=(STEPS,),
        in_specs=[
            pl.BlockSpec((TOK, w), lambda i: (0, i)),
            pl.BlockSpec((TOK, w), lambda i: (0, i)),
            pl.BlockSpec((TOK, B), lambda i: (0, 0)),
            pl.BlockSpec((TOK, B), lambda i: (0, 16)),
        ],
        out_specs=(
            pl.BlockSpec((128, w), first),
            pl.BlockSpec((128, w), first),
            pl.BlockSpec((B, w), lambda i: (0, jnp.maximum(i - STEPS // 2, 0))),
        ),
        name="product",
    )


def sum_y_kernel(keep_ref, left_ref, right_ref, out_ref):
    for k in range(4):
        at = slice(k * 512, (k + 1) * 512)
        out_ref[k, :128, :] = (keep_ref[:128, at].astype(F32) + left_ref[:, at].astype(F32)).astype(BF)
        out_ref[k, 128:, :] = (keep_ref[128:, at].astype(F32) + right_ref[:, at].astype(F32)).astype(BF)


def sum_y(keep, left, right):
    return call(
        sum_y_kernel,
        jax.ShapeDtypeStruct((4, B, 512), BF),
        (keep, left, right),
        8,
        TOK * D,
        3 * MB,
        in_specs=[VM] * 3,
        out_specs=VM,
        name="sum_y",
    )


def sum_y4_kernel(in_ref, gain_ref, send_ref, keep_ref):
    zh = lax.axis_index("zh")

    def total(z):
        at = aligned(z * B, B)
        s = in_ref[0, :, at].astype(F32)
        for k in range(1, 4):
            s = s + in_ref[k, :, at].astype(F32)
        return s

    send_ref[:B, :] = total(1 - zh).astype(BF)
    keep_ref[...] = total(zh)
    hi = gain_ref[...].astype(BF).astype(F32)
    mid = (gain_ref[...] - hi).astype(BF).astype(F32)
    low = gain_ref[...] - hi - mid
    row = lax.broadcasted_iota(jnp.int32, (8, B), 0)
    rows = jnp.where(row == 0, hi, jnp.where(row == 1, mid, jnp.where(row == 2, low, 0.0)))
    send_ref[B:, :] = rows.astype(BF)


def sum_y4(got, gain):
    return call(
        sum_y4_kernel,
        (jax.ShapeDtypeStruct((B + 8, B), BF), jax.ShapeDtypeStruct((B, B), F32)),
        (got, gain),
        6,
        TOK * D,
        2 * MB,
        in_specs=[VM, VM],
        out_specs=(VM, VM),
        name="sum_y4",
    )


def last_kernel(main_ref, keep_ref, got_ref, gain_ref, gain_main_ref, out_ref, gain_out_ref):
    n = NY * NH * NC
    s = keep_ref[...] + got_ref[:B, :].astype(F32)
    out_ref[...] = main_ref[...] + s.T / n
    got = jnp.sum(got_ref[B:, :].astype(F32), axis=0, keepdims=True)
    gain_out_ref[...] = gain_main_ref[...] + (gain_ref[...] + got) / n


def last(main, keep, got, gain, gain_main):
    return call(
        last_kernel,
        (jax.ShapeDtypeStruct((B, B), F32), jax.ShapeDtypeStruct((1, B), F32)),
        (main, keep, got, gain, gain_main),
        4,
        B * B * 4,
        MB,
        in_specs=[VM] * 5,
        out_specs=(VM, VM),
        name="last",
    )


def pairs(n, f):
    return [(i, f(i) % n) for i in range(n)]


def swap(v, axis, n, f):
    return lax.ppermute(v, axis, pairs(n, f))


def exchange(v, axis, **kw):
    return lax.all_to_all(v, axis, 0, 0, tiled=True, **kw)


def body(hidden, gain, weight, q_grad, q_main, gain_main):
    gain2 = gain.reshape(64, 128)
    part = partial(q_grad, weight, hidden, gain2)
    groups = [list(range(i * NG, (i + 1) * NG)) for i in range(NZ * NX // NG)]
    part = exchange(part, ("zl", "x"), axis_index_groups=groups)

    send, own, rinv = norm(hidden, gain2, q_grad)
    got = swap(send, "c", NC, lambda i: i ^ 1)
    left, right, keep = product(own, got, q_grad)
    left = swap(left, "y", NY, lambda i: i ^ 1)
    right = swap(right, "y", NY, lambda i: i + 1 if i % 2 else i - 1)

    send2, keep2 = sum_xz(part)
    got2 = swap(send2, "zl", NZ, lambda i: i ^ 2)

    four = sum_y(keep, left, right)
    four = exchange(four, "y", axis_index_groups=[[0, 2, 4, 6], [1, 3, 5, 7]])

    send3, keep3 = sum_z(keep2, got2, 2, 4)
    got3 = swap(send3, "zl", NZ, lambda i: i ^ 4)
    grad, own_gain = finish(keep3, got3, hidden, gain2, rinv)
    own_gain += swap(own_gain, "c", NC, lambda i: i ^ 1)
    own_gain += swap(own_gain, "y", NY, lambda i: i ^ 1)
    own_gain += swap(own_gain, "y", NY, lambda i: i ^ 2)
    own_gain += swap(own_gain, "y", NY, lambda i: i ^ 4)

    send_h, keep_h = sum_y4(four, own_gain)
    got_h = swap(send_h, "zh", NH, lambda i: i ^ 1)
    q_new, gain_new = last(q_main, keep_h, got_h, own_gain, gain_main.reshape(1, B))
    gain_new = gain_new.reshape(B)
    return grad, q_new, gain_new


def solution(mesh):
    fine = Mesh(mesh.devices.reshape(NY, NH, NC, NZ, NX), ("y", "zh", "c", "zl", "x"))
    dp, tp = ("y", "zh", "c"), ("zl", "x")
    in_specs = (P(dp, None), P(), P(None, tp), P(dp, tp), P(dp, tp), P(tp))
    out_specs = (P(dp, tp), P(dp, tp), P(tp))
    return jax.shard_map(body, mesh=fine, in_specs=in_specs, out_specs=out_specs, check_vma=False)
```

```python
import jax
import jax.numpy as jnp
from jax import lax
from jax.experimental import pallas as pl
from jax.experimental.pallas import tpu as pltpu
from jax.sharding import Mesh, PartitionSpec as P


BF = jnp.bfloat16
F32 = jnp.float32
NY, NH, NC, NZ, NX = 8, 2, 2, 8, 4
TOK = 128
D = 8192
B = 256
MB = 2**20
VM = pl.BlockSpec(memory_space=pltpu.VMEM)


def cost(flops, nbytes):
    return pl.CostEstimate(flops=flops, bytes_accessed=nbytes, transcendentals=0)


def params(mib):
    return pltpu.CompilerParams(vmem_limit_bytes=mib * MB if mib else None)


def call(kernel, out_shape, args, mib, flops, nbytes, **kw):
    return pl.pallas_call(
        kernel,
        out_shape=out_shape,
        compiler_params=params(mib),
        cost_estimate=cost(flops, nbytes),
        **kw,
    )(*args)


def aligned(start, size):
    return pl.ds(pl.multiple_of(start, size), size)


def two_rows(g_ref, block):
    at = lambda i: g_ref[pl.ds(2 * block + i, 1), :]
    return jnp.concatenate([at(0), at(1)], axis=1)


ROWS = 64


def norm_kernel(h_ref, g_ref, q_ref, send_ref, own_ref, rinv_ref, g32):
    par, core = lax.rem(lax.axis_index("y"), 2), lax.axis_index("c")
    g32[...] = g_ref[...].astype(F32)
    acc = jnp.zeros((ROWS, 128), F32)
    for j in range(D // 128):
        h = h_ref[:, j * 128 : (j + 1) * 128].astype(F32)
        acc = acc + h * h
    rinv = lax.rsqrt(jnp.sum(acc, axis=1, keepdims=True) / D + 1e-05)
    rinv_ref[...] = rinv
    for out, which in ((send_ref, 1 - core), (own_ref, core)):
        for j in range(16):
            o, k, zh = j // 8, (j // 2) % 4, j % 2
            y = 2 * k + (1 - par if o == 0 else par)
            block = y * 4 + zh * 2 + which
            h = h_ref[:, aligned(block * B, B)].astype(F32)
            out[:, j * B : (j + 1) * B] = (h * rinv * two_rows(g32, block)).astype(BF)
    send_ref[:, 16 * B :] = q_ref[...]


def norm(hidden, gain, q_grad):
    row = lambda n: pl.BlockSpec((ROWS, n), lambda i: (i, 0))
    return call(
        norm_kernel,
        (
            jax.ShapeDtypeStruct((TOK, 17 * B), BF),
            jax.ShapeDtypeStruct((TOK, 16 * B), BF),
            jax.ShapeDtypeStruct((TOK, 1), F32),
        ),
        (hidden, gain, q_grad),
        16,
        6 * TOK * D,
        4 * TOK * D,
        grid=(TOK // ROWS,),
        in_specs=[row(D), pl.BlockSpec((64, 128), lambda i: (0, 0)), row(B)],
        out_specs=(row(17 * B), row(16 * B), row(1)),
        scratch_shapes=[pltpu.VMEM((64, 128), F32)],
        name="norm",
    )


def eye():
    a = lax.broadcasted_iota(jnp.int32, (128, 128), 0)
    b = lax.broadcasted_iota(jnp.int32, (128, 128), 1)
    return a == b


def stat_rows(row):
    hi = row.astype(BF).astype(F32)
    both = jnp.concatenate([hi, row - hi], axis=1)
    first = lax.broadcasted_iota(jnp.int32, (8, 256), 0) == 0
    return jnp.where(first, jnp.broadcast_to(both, (8, 256)), 0.0).astype(BF)


def stat_of(block):
    both = jnp.sum(block.astype(F32), axis=0, keepdims=True)
    return both[:, :128] + both[:, 128:]


ZQ = NZ // 2
NG = 2 * NX
PIECE = ZQ * TOK + 8


def partial_kernel(q_ref, g_ref, w_hbm, h_hbm, out_hbm, w_ref, h_ref, out_ref, w_sem, h_sem, out_sem):
    wide = NX * B

    def w_copy(z):
        at = slice(z * wide, (z + 1) * wide)
        return pltpu.make_async_copy(w_hbm.at[at, :], w_ref.at[at, :], w_sem.at[z])

    def h_copy(z):
        at = slice(z * wide, (z + 1) * wide)
        return pltpu.make_async_copy(h_hbm.at[:, at], h_ref.at[:, at], h_sem.at[z])

    def out_copy(z, x):
        at = (z % 2 * NX + x, slice(z // 2 * TOK, (z // 2 + 1) * TOK))
        return pltpu.make_async_copy(out_ref.at[at], out_hbm.at[at], out_sem.at[z * NX + x])

    def stat_copy(d):
        at = (d, slice(ZQ * TOK, PIECE))
        return pltpu.make_async_copy(out_ref.at[at], out_hbm.at[at], out_sem.at[NZ * NX + d])

    for z in range(NZ):
        w_copy(z).start()
        h_copy(z).start()
    q = q_ref[...]
    g = g_ref[...].astype(F32)
    acc = jnp.zeros((TOK, 128), F32)
    for z in range(NZ):
        w_copy(z).wait()
        h_copy(z).wait()
        for x in range(NX):
            b = z * NX + x
            at = slice(b * B, (b + 1) * B)
            p = lax.dot_general(q, w_ref[at, :], (((1,), (1,)), ((), ())), preferred_element_type=F32)
            p = p.astype(BF)
            out_ref[z % 2 * NX + x, z // 2 * TOK : (z // 2 + 1) * TOK, :] = p
            t = p.astype(F32) * h_ref[:, at].astype(F32)
            acc = acc + t[:, :128] * g[2 * b : 2 * b + 1, :] + t[:, 128:] * g[2 * b + 1 : 2 * b + 2, :]
        if z > 0:
            for x in range(NX):
                out_copy(z - 1, x).start()
    s = jnp.sum(acc, axis=1, keepdims=True)
    rows = stat_rows(jnp.sum(jnp.where(eye(), s, 0.0), axis=0, keepdims=True))
    for d in range(NG):
        out_ref[d, ZQ * TOK :, :] = rows
    for x in range(NX):
        out_copy(NZ - 1, x).start()
    for d in range(NG):
        stat_copy(d).start()
    for z in range(NZ):
        for x in range(NX):
            out_copy(z, x).wait()
    for d in range(NG):
        stat_copy(d).wait()


HBM = pl.BlockSpec(memory_space=pltpu.HBM)


def partial(q_grad, weight, hidden, gain):
    return call(
        partial_kernel,
        jax.ShapeDtypeStruct((NG, PIECE, B), BF),
        (q_grad, gain, weight, hidden),
        None,
        2 * TOK * D * B,
        8 * MB,
        in_specs=[VM, VM, HBM, HBM],
        out_specs=HBM,
        scratch_shapes=[
            pltpu.VMEM((D, B), BF),
            pltpu.VMEM((TOK, D), BF),
            pltpu.VMEM((NG, PIECE, B), BF),
            pltpu.SemaphoreType.DMA((NZ,)),
            pltpu.SemaphoreType.DMA((NZ,)),
            pltpu.SemaphoreType.DMA((NZ * NX + NG,)),
        ],
        name="partial",
    )


def sum_xz_kernel(in_ref, out_ref):
    def total(at):
        s = in_ref[0, at, :].astype(F32)
        for d in range(1, NG):
            s = s + in_ref[d, at, :].astype(F32)
        return s

    rows = stat_rows(stat_of(total(slice(ZQ * TOK, PIECE))))
    for k in range(ZQ):
        out_ref[k, :TOK, :] = total(slice(k * TOK, (k + 1) * TOK)).astype(BF)
        out_ref[k, TOK:, :] = rows


def sum_xz(got):
    return call(
        sum_xz_kernel,
        jax.ShapeDtypeStruct((ZQ, TOK + 8, B), BF),
        (got,),
        12,
        TOK * D,
        4 * MB,
        in_specs=[VM],
        out_specs=VM,
        name="sum_xz",
    )


def finish_kernel(got_ref, h_ref, g_ref, rinv_ref, out_ref, gain_ref, g32):
    own = lax.axis_index("zl") * NX + lax.axis_index("x")
    g32[...] = g_ref[...].astype(F32)
    grad = got_ref[0, :TOK, :].astype(F32)
    stat = stat_of(got_ref[0, TOK:, :])
    for k in range(1, ZQ):
        grad = grad + got_ref[k, :TOK, :].astype(F32)
        stat = stat + stat_of(got_ref[k, TOK:, :])
    rinv = rinv_ref[...]
    stat = jnp.sum(jnp.where(eye(), stat, 0.0), axis=1, keepdims=True) * rinv / D
    xhat = h_ref[:, aligned(own * B, B)].astype(F32) * rinv
    gain_ref[...] = jnp.sum(grad * xhat, axis=0, keepdims=True)
    out_ref[...] = (rinv * (grad * two_rows(g32, own) - xhat * stat)).astype(BF)


def finish(got, hidden, gain, rinv):
    return call(
        finish_kernel,
        (jax.ShapeDtypeStruct((TOK, B), BF), jax.ShapeDtypeStruct((1, B), F32)),
        (got, hidden, gain, rinv),
        10,
        TOK * B * 16,
        MB,
        in_specs=[VM] * 4,
        out_specs=(VM, VM),
        scratch_shapes=[pltpu.VMEM((64, 128), F32)],
        name="finish",
    )


STEPS = 4


def product_kernel(own_ref, got_ref, q_ref, gq_ref, left_ref, right_ref, keep_ref):
    i = pl.program_id(0)
    a = jnp.concatenate([own_ref[...], got_ref[...]], axis=0)
    q = jnp.concatenate([q_ref[...], gq_ref[...]], axis=0)
    p = lax.dot_general(q, a, (((0,), (0,)), ((), ())), preferred_element_type=F32).astype(BF)

    @pl.when(i < STEPS // 2)
    def _():
        left_ref[...] = p[:128, :]
        right_ref[...] = p[128:, :]

    @pl.when(i >= STEPS // 2)
    def _():
        keep_ref[...] = p


def product(own, got, q_grad):
    w = 16 * B // STEPS
    half = jax.ShapeDtypeStruct((128, 8 * B), BF)
    first = lambda i: (0, jnp.minimum(i, STEPS // 2 - 1))
    return call(
        product_kernel,
        (half, half, jax.ShapeDtypeStruct((B, 8 * B), BF)),
        (own, got, q_grad, got),
        16,
        2 * TOK * D * B,
        4 * MB,
        grid=(STEPS,),
        in_specs=[
            pl.BlockSpec((TOK, w), lambda i: (0, i)),
            pl.BlockSpec((TOK, w), lambda i: (0, i)),
            pl.BlockSpec((TOK, B), lambda i: (0, 0)),
            pl.BlockSpec((TOK, B), lambda i: (0, 16)),
        ],
        out_specs=(
            pl.BlockSpec((128, w), first),
            pl.BlockSpec((128, w), first),
            pl.BlockSpec((B, w), lambda i: (0, jnp.maximum(i - STEPS // 2, 0))),
        ),
        name="product",
    )


def sum_y_kernel(keep_ref, left_ref, right_ref, out_ref):
    for k in range(4):
        at = slice(k * 512, (k + 1) * 512)
        out_ref[k, :128, :] = (keep_ref[:128, at].astype(F32) + left_ref[:, at].astype(F32)).astype(BF)
        out_ref[k, 128:, :] = (keep_ref[128:, at].astype(F32) + right_ref[:, at].astype(F32)).astype(BF)


def sum_y(keep, left, right):
    return call(
        sum_y_kernel,
        jax.ShapeDtypeStruct((4, B, 512), BF),
        (keep, left, right),
        8,
        TOK * D,
        3 * MB,
        in_specs=[VM] * 3,
        out_specs=VM,
        name="sum_y",
    )


def sum_y4_kernel(in_ref, send_ref, keep_ref):
    zh = lax.axis_index("zh")

    def total(z):
        at = aligned(z * B, B)
        s = in_ref[0, :, at].astype(F32)
        for k in range(1, 4):
            s = s + in_ref[k, :, at].astype(F32)
        return s

    send_ref[...] = total(1 - zh).astype(BF)
    keep_ref[...] = total(zh)


def sum_y4(got):
    return call(
        sum_y4_kernel,
        (jax.ShapeDtypeStruct((B, B), BF), jax.ShapeDtypeStruct((B, B), F32)),
        (got,),
        6,
        TOK * D,
        2 * MB,
        in_specs=[VM],
        out_specs=(VM, VM),
        name="sum_y4",
    )


def last_kernel(main_ref, keep_ref, got_ref, out_ref):
    s = keep_ref[...] + got_ref[...].astype(F32)
    out_ref[...] = main_ref[...] + s.T / (NY * NH * NC)


def last(main, keep, got):
    return call(
        last_kernel,
        jax.ShapeDtypeStruct((B, B), F32),
        (main, keep, got),
        4,
        B * B * 4,
        MB,
        in_specs=[VM] * 3,
        out_specs=VM,
        name="last",
    )


def pairs(n, f):
    return [(i, f(i) % n) for i in range(n)]


def swap(v, axis, n, f):
    return lax.ppermute(v, axis, pairs(n, f))


def exchange(v, axis, **kw):
    return lax.all_to_all(v, axis, 0, 0, tiled=True, **kw)


def body(hidden, gain, weight, q_grad, q_main, gain_main):
    gain2 = gain.reshape(64, 128)
    part = partial(q_grad, weight, hidden, gain2)
    groups = [list(range(i * NG, (i + 1) * NG)) for i in range(NZ * NX // NG)]
    part = exchange(part, ("zl", "x"), axis_index_groups=groups)

    send, own, rinv = norm(hidden, gain2, q_grad)
    got = swap(send, "c", NC, lambda i: i ^ 1)
    left, right, keep = product(own, got, q_grad)
    left = swap(left, "y", NY, lambda i: i ^ 1)
    right = swap(right, "y", NY, lambda i: i + 1 if i % 2 else i - 1)

    evens_odds = [[0, 2, 4, 6], [1, 3, 5, 7]]
    part = exchange(sum_xz(part), "zl", axis_index_groups=evens_odds)
    grad, own_gain = finish(part, hidden, gain2, rinv)

    four = exchange(sum_y(keep, left, right), "y", axis_index_groups=evens_odds)
    got_gain = swap(own_gain, "zh", NH, lambda i: i ^ 1)

    send_h, keep_h = sum_y4(four)
    got_h = swap(send_h, "zh", NH, lambda i: i ^ 1)
    all_gain = jnp.broadcast_to((own_gain + got_gain)[None], (NY * NC, 1, B))
    all_gain = exchange(all_gain, ("y", "c"))
    q_new = last(q_main, keep_h, got_h)
    gain_new = gain_main + jnp.sum(all_gain, axis=(0, 1)) / (NY * NH * NC)
    return grad, q_new, gain_new


def solution(mesh):
    fine = Mesh(mesh.devices.reshape(NY, NH, NC, NZ, NX), ("y", "zh", "c", "zl", "x"))
    dp, tp = ("y", "zh", "c"), ("zl", "x")
    in_specs = (P(dp, None), P(), P(None, tp), P(dp, tp), P(dp, tp), P(tp))
    out_specs = (P(dp, tp), P(dp, tp), P(tp))
    return jax.shard_map(body, mesh=fine, in_specs=in_specs, out_specs=out_specs, check_vma=False)
```

```python
import functools

import jax
import jax.numpy as jnp
from jax import lax
from jax.experimental import pallas as pl
from jax.experimental.pallas import tpu as pltpu
from jax.sharding import Mesh, PartitionSpec as P


BF = jnp.bfloat16
F32 = jnp.float32
NY, NH, NC, NZ, NX = 8, 2, 2, 8, 4
TOK = 128
D = 8192
B = 256
MB = 2**20
VM = pl.BlockSpec(memory_space=pltpu.VMEM)


def cost(flops, nbytes):
    return pl.CostEstimate(flops=flops, bytes_accessed=nbytes, transcendentals=0)


def params(mib):
    return pltpu.CompilerParams(vmem_limit_bytes=mib * MB if mib else None)


def call(kernel, out_shape, args, mib, flops, nbytes, **kw):
    return pl.pallas_call(
        kernel,
        out_shape=out_shape,
        compiler_params=params(mib),
        cost_estimate=cost(flops, nbytes),
        **kw,
    )(*args)


def aligned(start, size):
    return pl.ds(pl.multiple_of(start, size), size)


def two_rows(g_ref, block):
    at = lambda i: g_ref[pl.ds(2 * block + i, 1), :]
    return jnp.concatenate([at(0), at(1)], axis=1)


ROWS = 64


def norm_kernel(h_ref, g_ref, q_ref, send_ref, own_ref, rinv_ref, g32):
    par, core = lax.rem(lax.axis_index("y"), 2), lax.axis_index("c")
    g32[...] = g_ref[...].astype(F32)
    acc = jnp.zeros((ROWS, 128), F32)
    for j in range(D // 128):
        h = h_ref[:, j * 128 : (j + 1) * 128].astype(F32)
        acc = acc + h * h
    rinv = lax.rsqrt(jnp.sum(acc, axis=1, keepdims=True) / D + 1e-05)
    rinv_ref[...] = rinv
    for out, which in ((send_ref, 1 - core), (own_ref, core)):
        for j in range(16):
            o, k, zh = j // 8, (j // 2) % 4, j % 2
            y = 2 * k + (1 - par if o == 0 else par)
            block = y * 4 + zh * 2 + which
            h = h_ref[:, aligned(block * B, B)].astype(F32)
            out[:, j * B : (j + 1) * B] = (h * rinv * two_rows(g32, block)).astype(BF)
    send_ref[:, 16 * B :] = q_ref[...]


def norm(hidden, gain, q_grad):
    row = lambda n: pl.BlockSpec((ROWS, n), lambda i: (i, 0))
    return call(
        norm_kernel,
        (
            jax.ShapeDtypeStruct((TOK, 17 * B), BF),
            jax.ShapeDtypeStruct((TOK, 16 * B), BF),
            jax.ShapeDtypeStruct((TOK, 1), F32),
        ),
        (hidden, gain, q_grad),
        16,
        6 * TOK * D,
        4 * TOK * D,
        grid=(TOK // ROWS,),
        in_specs=[row(D), pl.BlockSpec((64, 128), lambda i: (0, 0)), row(B)],
        out_specs=(row(17 * B), row(16 * B), row(1)),
        scratch_shapes=[pltpu.VMEM((64, 128), F32)],
        name="norm",
    )


def eye():
    a = lax.broadcasted_iota(jnp.int32, (128, 128), 0)
    b = lax.broadcasted_iota(jnp.int32, (128, 128), 1)
    return a == b


def stat_rows(row):
    hi = row.astype(BF).astype(F32)
    both = jnp.concatenate([hi, row - hi], axis=1)
    first = lax.broadcasted_iota(jnp.int32, (8, 256), 0) == 0
    return jnp.where(first, jnp.broadcast_to(both, (8, 256)), 0.0).astype(BF)


def stat_of(block):
    both = jnp.sum(block.astype(F32), axis=0, keepdims=True)
    return both[:, :128] + both[:, 128:]


ZQ = NZ // 2
NG = 2 * NX
PIECE = ZQ * TOK + 8


def partial_kernel(q_ref, g_ref, w_hbm, h_hbm, out_hbm, w_ref, h_ref, out_ref, w_sem, h_sem, out_sem):
    wide = NX * B

    def w_copy(z):
        at = slice(z * wide, (z + 1) * wide)
        return pltpu.make_async_copy(w_hbm.at[at, :], w_ref.at[at, :], w_sem.at[z])

    def h_copy(z):
        at = slice(z * wide, (z + 1) * wide)
        return pltpu.make_async_copy(h_hbm.at[:, at], h_ref.at[:, at], h_sem.at[z])

    def out_copy(z, x):
        at = (z % 2 * NX + x, slice(z // 2 * TOK, (z // 2 + 1) * TOK))
        return pltpu.make_async_copy(out_ref.at[at], out_hbm.at[at], out_sem.at[z * NX + x])

    def stat_copy(d):
        at = (d, slice(ZQ * TOK, PIECE))
        return pltpu.make_async_copy(out_ref.at[at], out_hbm.at[at], out_sem.at[NZ * NX + d])

    for z in range(NZ):
        w_copy(z).start()
        h_copy(z).start()
    q = q_ref[...]
    g = g_ref[...].astype(F32)
    acc = jnp.zeros((TOK, 128), F32)
    for z in range(NZ):
        w_copy(z).wait()
        h_copy(z).wait()
        for x in range(NX):
            b = z * NX + x
            at = slice(b * B, (b + 1) * B)
            p = lax.dot_general(q, w_ref[at, :], (((1,), (1,)), ((), ())), preferred_element_type=F32)
            p = p.astype(BF)
            out_ref[z % 2 * NX + x, z // 2 * TOK : (z // 2 + 1) * TOK, :] = p
            t = p.astype(F32) * h_ref[:, at].astype(F32)
            acc = acc + t[:, :128] * g[2 * b : 2 * b + 1, :] + t[:, 128:] * g[2 * b + 1 : 2 * b + 2, :]
        if z > 0:
            for x in range(NX):
                out_copy(z - 1, x).start()
    s = jnp.sum(acc, axis=1, keepdims=True)
    rows = stat_rows(jnp.sum(jnp.where(eye(), s, 0.0), axis=0, keepdims=True))
    for d in range(NG):
        out_ref[d, ZQ * TOK :, :] = rows
    for x in range(NX):
        out_copy(NZ - 1, x).start()
    for d in range(NG):
        stat_copy(d).start()
    for z in range(NZ):
        for x in range(NX):
            out_copy(z, x).wait()
    for d in range(NG):
        stat_copy(d).wait()


HBM = pl.BlockSpec(memory_space=pltpu.HBM)


def partial(q_grad, weight, hidden, gain):
    return call(
        partial_kernel,
        jax.ShapeDtypeStruct((NG, PIECE, B), BF),
        (q_grad, gain, weight, hidden),
        None,
        2 * TOK * D * B,
        8 * MB,
        in_specs=[VM, VM, HBM, HBM],
        out_specs=HBM,
        scratch_shapes=[
            pltpu.VMEM((D, B), BF),
            pltpu.VMEM((TOK, D), BF),
            pltpu.VMEM((NG, PIECE, B), BF),
            pltpu.SemaphoreType.DMA((NZ,)),
            pltpu.SemaphoreType.DMA((NZ,)),
            pltpu.SemaphoreType.DMA((NZ * NX + NG,)),
        ],
        name="partial",
    )


def sum_xz_kernel(in_ref, send_ref, keep_ref):
    bit = lax.rem(lax.div(lax.axis_index("zl"), 2), 2)

    def total(at):
        s = in_ref[0, at, :].astype(F32)
        for d in range(1, NG):
            s = s + in_ref[d, at, :].astype(F32)
        return s

    rows = stat_rows(stat_of(total(slice(ZQ * TOK, PIECE))))
    for k in range(ZQ // 2):
        at = slice(k * TOK, (k + 1) * TOK)
        send_ref[at, :] = total(aligned((2 * k + 1 - bit) * TOK, TOK)).astype(BF)
        keep_ref[at, :] = total(aligned((2 * k + bit) * TOK, TOK))
    send_ref[ZQ // 2 * TOK :, :] = rows
    keep_ref[ZQ // 2 * TOK :, :] = rows.astype(F32)


def sum_xz(got):
    rows = ZQ // 2 * TOK + 8
    return call(
        sum_xz_kernel,
        (jax.ShapeDtypeStruct((rows, B), BF), jax.ShapeDtypeStruct((rows, B), F32)),
        (got,),
        12,
        TOK * D,
        4 * MB,
        in_specs=[VM],
        out_specs=(VM, VM),
        name="sum_xz",
    )


def sum_z_kernel(count, shift, keep_ref, got_ref, send_ref, out_ref):
    bit = lax.rem(lax.div(lax.axis_index("zl"), shift), 2)
    half = count // 2

    def total(at):
        return keep_ref[at, :] + got_ref[at, :].astype(F32)

    for k in range(half):
        at = slice(k * TOK, (k + 1) * TOK)
        send_ref[at, :] = total(aligned((2 * k + 1 - bit) * TOK, TOK)).astype(BF)
    rows = stat_rows(stat_of(total(slice(count * TOK, count * TOK + 8))))
    send_ref[half * TOK :, :] = rows
    for k in range(half):
        at = slice(k * TOK, (k + 1) * TOK)
        out_ref[at, :] = total(aligned((2 * k + bit) * TOK, TOK))
    out_ref[half * TOK :, :] = rows.astype(F32)


def sum_z(keep, got, count, shift):
    rows = count // 2 * TOK + 8
    return call(
        functools.partial(sum_z_kernel, count, shift),
        (jax.ShapeDtypeStruct((rows, B), BF), jax.ShapeDtypeStruct((rows, B), F32)),
        (keep, got),
        6,
        count * TOK * B,
        count * MB // 2,
        in_specs=[VM, VM],
        out_specs=(VM, VM),
        name=f"sum_z{shift}",
    )


def finish_kernel(keep_ref, got_ref, h_ref, g_ref, rinv_ref, out_ref, gain_ref, g32):
    own = lax.axis_index("zl") * NX + lax.axis_index("x")
    g32[...] = g_ref[...].astype(F32)
    grad = keep_ref[:TOK, :] + got_ref[:TOK, :].astype(F32)
    stat = stat_of(keep_ref[TOK:, :] + got_ref[TOK:, :].astype(F32))
    rinv = rinv_ref[...]
    stat = jnp.sum(jnp.where(eye(), stat, 0.0), axis=1, keepdims=True) * rinv / D
    xhat = h_ref[:, aligned(own * B, B)].astype(F32) * rinv
    gain_ref[...] = jnp.sum(grad * xhat, axis=0, keepdims=True)
    out_ref[...] = (rinv * (grad * two_rows(g32, own) - xhat * stat)).astype(BF)


def finish(keep, got, hidden, gain, rinv):
    return call(
        finish_kernel,
        (
            jax.ShapeDtypeStruct((TOK, B), BF),
            jax.ShapeDtypeStruct((1, B), F32),
        ),
        (keep, got, hidden, gain, rinv),
        10,
        TOK * B * 16,
        MB,
        in_specs=[VM] * 5,
        out_specs=(VM, VM),
        scratch_shapes=[pltpu.VMEM((64, 128), F32)],
        name="finish",
    )


STEPS = 4


def product_kernel(own_ref, got_ref, q_ref, gq_ref, left_ref, right_ref, keep_ref):
    i = pl.program_id(0)
    a = jnp.concatenate([own_ref[...], got_ref[...]], axis=0)
    q = jnp.concatenate([q_ref[...], gq_ref[...]], axis=0)
    p = lax.dot_general(q, a, (((0,), (0,)), ((), ())), preferred_element_type=F32).astype(BF)

    @pl.when(i < STEPS // 2)
    def _():
        left_ref[...] = p[:128, :]
        right_ref[...] = p[128:, :]

    @pl.when(i >= STEPS // 2)
    def _():
        keep_ref[...] = p


def product(own, got, q_grad):
    w = 16 * B // STEPS
    half = jax.ShapeDtypeStruct((128, 8 * B), BF)
    first = lambda i: (0, jnp.minimum(i, STEPS // 2 - 1))
    return call(
        product_kernel,
        (half, half, jax.ShapeDtypeStruct((B, 8 * B), BF)),
        (own, got, q_grad, got),
        16,
        2 * TOK * D * B,
        4 * MB,
        grid=(STEPS,),
        in_specs=[
            pl.BlockSpec((TOK, w), lambda i: (0, i)),
            pl.BlockSpec((TOK, w), lambda i: (0, i)),
            pl.BlockSpec((TOK, B), lambda i: (0, 0)),
            pl.BlockSpec((TOK, B), lambda i: (0, 16)),
        ],
        out_specs=(
            pl.BlockSpec((128, w), first),
            pl.BlockSpec((128, w), first),
            pl.BlockSpec((B, w), lambda i: (0, jnp.maximum(i - STEPS // 2, 0))),
        ),
        name="product",
    )


def sum_y_kernel(keep_ref, left_ref, right_ref, out_ref):
    for k in range(4):
        at = slice(k * 512, (k + 1) * 512)
        out_ref[k, :128, :] = (keep_ref[:128, at].astype(F32) + left_ref[:, at].astype(F32)).astype(BF)
        out_ref[k, 128:, :] = (keep_ref[128:, at].astype(F32) + right_ref[:, at].astype(F32)).astype(BF)


def sum_y(keep, left, right):
    return call(
        sum_y_kernel,
        jax.ShapeDtypeStruct((4, B, 512), BF),
        (keep, left, right),
        8,
        TOK * D,
        3 * MB,
        in_specs=[VM] * 3,
        out_specs=VM,
        name="sum_y",
    )


def sum_y4_kernel(in_ref, send_ref, keep_ref):
    zh = lax.axis_index("zh")

    def total(z):
        at = aligned(z * B, B)
        s = in_ref[0, :, at].astype(F32)
        for k in range(1, 4):
            s = s + in_ref[k, :, at].astype(F32)
        return s

    send_ref[...] = total(1 - zh).astype(BF)
    keep_ref[...] = total(zh)


def sum_y4(got):
    return call(
        sum_y4_kernel,
        (jax.ShapeDtypeStruct((B, B), BF), jax.ShapeDtypeStruct((B, B), F32)),
        (got,),
        6,
        TOK * D,
        2 * MB,
        in_specs=[VM],
        out_specs=(VM, VM),
        name="sum_y4",
    )


def last_kernel(main_ref, keep_ref, got_ref, out_ref):
    s = keep_ref[...] + got_ref[...].astype(F32)
    out_ref[...] = main_ref[...] + s.T / (NY * NH * NC)


def last(main, keep, got):
    return call(
        last_kernel,
        jax.ShapeDtypeStruct((B, B), F32),
        (main, keep, got),
        4,
        B * B * 4,
        MB,
        in_specs=[VM] * 3,
        out_specs=VM,
        name="last",
    )


def gain_mix_kernel(own_ref, got_ref, out_ref):
    total = own_ref[...] + got_ref[...]
    for i in range(NY * NC):
        out_ref[i] = total


def gain_mix(own, got):
    return call(
        gain_mix_kernel,
        jax.ShapeDtypeStruct((NY * NC, 1, B), F32),
        (own, got),
        4,
        B,
        MB // 16,
        in_specs=[VM] * 2,
        out_specs=VM,
        name="gain_mix",
    )


def pairs(n, f):
    return [(i, f(i) % n) for i in range(n)]


def swap(v, axis, n, f):
    return lax.ppermute(v, axis, pairs(n, f))


def exchange(v, axis, **kw):
    return lax.all_to_all(v, axis, 0, 0, tiled=True, **kw)


def body(hidden, gain, weight, q_grad, q_main, gain_main):
    gain2 = gain.reshape(64, 128)
    part = partial(q_grad, weight, hidden, gain2)
    groups = [list(range(i * NG, (i + 1) * NG)) for i in range(NZ * NX // NG)]
    part = exchange(part, ("zl", "x"), axis_index_groups=groups)

    send, own, rinv = norm(hidden, gain2, q_grad)
    got = swap(send, "c", NC, lambda i: i ^ 1)
    left, right, keep = product(own, got, q_grad)
    left = swap(left, "y", NY, lambda i: i ^ 1)
    right = swap(right, "y", NY, lambda i: i + 1 if i % 2 else i - 1)

    send2, keep2 = sum_xz(part)
    got2 = swap(send2, "zl", NZ, lambda i: i ^ 2)

    four = sum_y(keep, left, right)
    four = exchange(four, "y", axis_index_groups=[[0, 2, 4, 6], [1, 3, 5, 7]])

    send3, keep3 = sum_z(keep2, got2, 2, 4)
    got3 = swap(send3, "zl", NZ, lambda i: i ^ 4)
    grad, own_gain = finish(keep3, got3, hidden, gain2, rinv)
    got_gain = swap(own_gain, "zh", NH, lambda i: i ^ 1)

    send_h, keep_h = sum_y4(four)
    got_h = swap(send_h, "zh", NH, lambda i: i ^ 1)
    all_gain = exchange(gain_mix(own_gain, got_gain), ("y", "c"))
    q_new = last(q_main, keep_h, got_h)
    gain_new = gain_main + jnp.sum(all_gain, axis=(0, 1)) / (NY * NH * NC)
    return grad, q_new, gain_new


def solution(mesh):
    fine = Mesh(mesh.devices.reshape(NY, NH, NC, NZ, NX), ("y", "zh", "c", "zl", "x"))
    dp, tp = ("y", "zh", "c"), ("zl", "x")
    in_specs = (P(dp, None), P(), P(None, tp), P(dp, tp), P(dp, tp), P(tp))
    out_specs = (P(dp, tp), P(dp, tp), P(tp))
    return jax.shard_map(body, mesh=fine, in_specs=in_specs, out_specs=out_specs, check_vma=False)
```

```python
import functools

import jax
import jax.numpy as jnp
from jax import lax
from jax.experimental import pallas as pl
from jax.experimental.pallas import tpu as pltpu
from jax.sharding import Mesh, PartitionSpec as P


BF = jnp.bfloat16
F32 = jnp.float32
NY, NH, NC, NZ, NX = 8, 2, 2, 8, 4
TOK = 128
D = 8192
B = 256
MB = 2**20
VM = pl.BlockSpec(memory_space=pltpu.VMEM)


def cost(flops, nbytes):
    return pl.CostEstimate(flops=flops, bytes_accessed=nbytes, transcendentals=0)


def params(mib):
    return pltpu.CompilerParams(vmem_limit_bytes=mib * MB if mib else None)


def call(kernel, out_shape, args, mib, flops, nbytes, **kw):
    return pl.pallas_call(
        kernel,
        out_shape=out_shape,
        compiler_params=params(mib),
        cost_estimate=cost(flops, nbytes),
        **kw,
    )(*args)


def aligned(start, size):
    return pl.ds(pl.multiple_of(start, size), size)


def two_rows(g_ref, block):
    at = lambda i: g_ref[pl.ds(2 * block + i, 1), :]
    return jnp.concatenate([at(0), at(1)], axis=1)


ROWS = 64


def norm_kernel(h_ref, g_ref, q_ref, send_ref, own_ref, rinv_ref, g32):
    par, core = lax.rem(lax.axis_index("y"), 2), lax.axis_index("c")
    g32[...] = g_ref[...].astype(F32)
    acc = jnp.zeros((ROWS, 128), F32)
    for j in range(D // 128):
        h = h_ref[:, j * 128 : (j + 1) * 128].astype(F32)
        acc = acc + h * h
    rinv = lax.rsqrt(jnp.sum(acc, axis=1, keepdims=True) / D + 1e-05)
    rinv_ref[...] = rinv
    for out, which in ((send_ref, 1 - core), (own_ref, core)):
        for j in range(16):
            o, k, zh = j // 8, (j // 2) % 4, j % 2
            y = 2 * k + (1 - par if o == 0 else par)
            block = y * 4 + zh * 2 + which
            h = h_ref[:, aligned(block * B, B)].astype(F32)
            out[:, j * B : (j + 1) * B] = (h * rinv * two_rows(g32, block)).astype(BF)
    send_ref[:, 16 * B :] = q_ref[...]


def norm(hidden, gain, q_grad):
    row = lambda n: pl.BlockSpec((ROWS, n), lambda i: (i, 0))
    return call(
        norm_kernel,
        (
            jax.ShapeDtypeStruct((TOK, 17 * B), BF),
            jax.ShapeDtypeStruct((TOK, 16 * B), BF),
            jax.ShapeDtypeStruct((TOK, 1), F32),
        ),
        (hidden, gain, q_grad),
        56,
        6 * TOK * D,
        4 * TOK * D,
        grid=(TOK // ROWS,),
        in_specs=[row(D), pl.BlockSpec((64, 128), lambda i: (0, 0)), row(B)],
        out_specs=(row(17 * B), row(16 * B), row(1)),
        scratch_shapes=[pltpu.VMEM((64, 128), F32)],
        name="norm",
    )


def eye():
    a = lax.broadcasted_iota(jnp.int32, (128, 128), 0)
    b = lax.broadcasted_iota(jnp.int32, (128, 128), 1)
    return a == b


def stat_rows(row):
    hi = row.astype(BF).astype(F32)
    both = jnp.concatenate([hi, row - hi], axis=1)
    first = lax.broadcasted_iota(jnp.int32, (8, 256), 0) == 0
    return jnp.where(first, jnp.broadcast_to(both, (8, 256)), 0.0).astype(BF)


def stat_of(block):
    both = jnp.sum(block.astype(F32), axis=0, keepdims=True)
    return both[:, :128] + both[:, 128:]


ZQ = NZ // 2
NG = 2 * NX
PIECE = ZQ * TOK + 8


def partial_kernel(q_ref, g_ref, w_hbm, h_hbm, out_hbm, w_ref, h_ref, out_ref, w_sem, h_sem, out_sem):
    wide = NX * B

    def w_copy(z):
        at = slice(z * wide, (z + 1) * wide)
        return pltpu.make_async_copy(w_hbm.at[at, :], w_ref.at[at, :], w_sem.at[z])

    def h_copy(z):
        at = slice(z * wide, (z + 1) * wide)
        return pltpu.make_async_copy(h_hbm.at[:, at], h_ref.at[:, at], h_sem.at[z])

    def out_copy(z, x):
        at = (z % 2 * NX + x, slice(z // 2 * TOK, (z // 2 + 1) * TOK))
        return pltpu.make_async_copy(out_ref.at[at], out_hbm.at[at], out_sem.at[z * NX + x])

    def stat_copy(d):
        at = (d, slice(ZQ * TOK, PIECE))
        return pltpu.make_async_copy(out_ref.at[at], out_hbm.at[at], out_sem.at[NZ * NX + d])

    for z in range(NZ):
        w_copy(z).start()
        h_copy(z).start()
    q = q_ref[...]
    g = g_ref[...].astype(F32)
    acc = jnp.zeros((TOK, 128), F32)
    for z in range(NZ):
        w_copy(z).wait()
        h_copy(z).wait()
        for x in range(NX):
            b = z * NX + x
            at = slice(b * B, (b + 1) * B)
            p = lax.dot_general(q, w_ref[at, :], (((1,), (1,)), ((), ())), preferred_element_type=F32)
            p = p.astype(BF)
            out_ref[z % 2 * NX + x, z // 2 * TOK : (z // 2 + 1) * TOK, :] = p
            t = p.astype(F32) * h_ref[:, at].astype(F32)
            acc = acc + t[:, :128] * g[2 * b : 2 * b + 1, :] + t[:, 128:] * g[2 * b + 1 : 2 * b + 2, :]
        if z > 0:
            for x in range(NX):
                out_copy(z - 1, x).start()
    s = jnp.sum(acc, axis=1, keepdims=True)
    rows = stat_rows(jnp.sum(jnp.where(eye(), s, 0.0), axis=0, keepdims=True))
    for d in range(NG):
        out_ref[d, ZQ * TOK :, :] = rows
    for x in range(NX):
        out_copy(NZ - 1, x).start()
    for d in range(NG):
        stat_copy(d).start()
    for z in range(NZ):
        for x in range(NX):
            out_copy(z, x).wait()
    for d in range(NG):
        stat_copy(d).wait()


HBM = pl.BlockSpec(memory_space=pltpu.HBM)


def partial(q_grad, weight, hidden, gain):
    return call(
        partial_kernel,
        jax.ShapeDtypeStruct((NG, PIECE, B), BF),
        (q_grad, gain, weight, hidden),
        None,
        2 * TOK * D * B,
        8 * MB,
        in_specs=[VM, VM, HBM, HBM],
        out_specs=HBM,
        scratch_shapes=[
            pltpu.VMEM((D, B), BF),
            pltpu.VMEM((TOK, D), BF),
            pltpu.VMEM((NG, PIECE, B), BF),
            pltpu.SemaphoreType.DMA((NZ,)),
            pltpu.SemaphoreType.DMA((NZ,)),
            pltpu.SemaphoreType.DMA((NZ * NX + NG,)),
        ],
        name="partial",
    )


def sum_xz_kernel(in_ref, send_ref, keep_ref):
    bit = lax.rem(lax.div(lax.axis_index("zl"), 2), 2)

    def total(at):
        s = in_ref[0, at, :].astype(F32)
        for d in range(1, NG):
            s = s + in_ref[d, at, :].astype(F32)
        return s

    rows = stat_rows(stat_of(total(slice(ZQ * TOK, PIECE))))
    for k in range(ZQ // 2):
        at = slice(k * TOK, (k + 1) * TOK)
        send_ref[at, :] = total(aligned((2 * k + 1 - bit) * TOK, TOK)).astype(BF)
        keep_ref[at, :] = total(aligned((2 * k + bit) * TOK, TOK))
    send_ref[ZQ // 2 * TOK :, :] = rows
    keep_ref[ZQ // 2 * TOK :, :] = rows.astype(F32)


def sum_xz(got):
    rows = ZQ // 2 * TOK + 8
    return call(
        sum_xz_kernel,
        (jax.ShapeDtypeStruct((rows, B), BF), jax.ShapeDtypeStruct((rows, B), F32)),
        (got,),
        12,
        TOK * D,
        4 * MB,
        in_specs=[VM],
        out_specs=(VM, VM),
        name="sum_xz",
    )


def sum_z_kernel(count, shift, keep_ref, got_ref, send_ref, out_ref):
    bit = lax.rem(lax.div(lax.axis_index("zl"), shift), 2)
    half = count // 2

    def total(at):
        return keep_ref[at, :] + got_ref[at, :].astype(F32)

    for k in range(half):
        at = slice(k * TOK, (k + 1) * TOK)
        send_ref[at, :] = total(aligned((2 * k + 1 - bit) * TOK, TOK)).astype(BF)
    rows = stat_rows(stat_of(total(slice(count * TOK, count * TOK + 8))))
    send_ref[half * TOK :, :] = rows
    for k in range(half):
        at = slice(k * TOK, (k + 1) * TOK)
        out_ref[at, :] = total(aligned((2 * k + bit) * TOK, TOK))
    out_ref[half * TOK :, :] = rows.astype(F32)


def sum_z(keep, got, count, shift):
    rows = count // 2 * TOK + 8
    return call(
        functools.partial(sum_z_kernel, count, shift),
        (jax.ShapeDtypeStruct((rows, B), BF), jax.ShapeDtypeStruct((rows, B), F32)),
        (keep, got),
        6,
        count * TOK * B,
        count * MB // 2,
        in_specs=[VM, VM],
        out_specs=(VM, VM),
        name=f"sum_z{shift}",
    )


def finish_kernel(keep_ref, got_ref, h_ref, g_ref, rinv_ref, out_ref, gain_ref, g32):
    own = lax.axis_index("zl") * NX + lax.axis_index("x")
    g32[...] = g_ref[...].astype(F32)
    grad = keep_ref[:TOK, :] + got_ref[:TOK, :].astype(F32)
    stat = stat_of(keep_ref[TOK:, :] + got_ref[TOK:, :].astype(F32))
    rinv = rinv_ref[...]
    stat = jnp.sum(jnp.where(eye(), stat, 0.0), axis=1, keepdims=True) * rinv / D
    xhat = h_ref[:, aligned(own * B, B)].astype(F32) * rinv
    gain_ref[...] = jnp.sum(grad * xhat, axis=0, keepdims=True)
    out_ref[...] = (rinv * (grad * two_rows(g32, own) - xhat * stat)).astype(BF)


def finish(keep, got, hidden, gain, rinv):
    return call(
        finish_kernel,
        (
            jax.ShapeDtypeStruct((TOK, B), BF),
            jax.ShapeDtypeStruct((1, B), F32),
        ),
        (keep, got, hidden, gain, rinv),
        10,
        TOK * B * 16,
        MB,
        in_specs=[VM] * 5,
        out_specs=(VM, VM),
        scratch_shapes=[pltpu.VMEM((64, 128), F32)],
        name="finish",
    )


STEPS = 2


def product_of(own_ref, got_ref, q_ref, gq_ref):
    a = jnp.concatenate([own_ref[...], got_ref[...]], axis=0)
    q = jnp.concatenate([q_ref[...], gq_ref[...]], axis=0)
    return lax.dot_general(q, a, (((0,), (0,)), ((), ())), preferred_element_type=F32).astype(BF)


def sent_kernel(own_ref, got_ref, q_ref, gq_ref, left_ref, right_ref):
    p = product_of(own_ref, got_ref, q_ref, gq_ref)
    left_ref[...] = p[:128, :]
    right_ref[...] = p[128:, :]


def kept_kernel(own_ref, got_ref, q_ref, gq_ref, keep_ref):
    keep_ref[...] = product_of(own_ref, got_ref, q_ref, gq_ref)


def product(kernel, own, got, q_grad, first, rows, name):
    w = 8 * B // STEPS
    shape = tuple(jax.ShapeDtypeStruct((r, 8 * B), BF) for r in rows)
    return call(
        kernel,
        shape,
        (own, got, q_grad, got),
        16,
        TOK * D * B,
        2 * MB,
        grid=(STEPS,),
        in_specs=[
            pl.BlockSpec((TOK, w), lambda i: (0, i + first)),
            pl.BlockSpec((TOK, w), lambda i: (0, i + first)),
            pl.BlockSpec((TOK, B), lambda i: (0, 0)),
            pl.BlockSpec((TOK, B), lambda i: (0, 16)),
        ],
        out_specs=tuple(pl.BlockSpec((r, w), lambda i: (0, i)) for r in rows),
        name=name,
    )


def sum_y_kernel(keep_ref, left_ref, right_ref, out_ref):
    for k in range(4):
        at = slice(k * 512, (k + 1) * 512)
        out_ref[k, :128, :] = (keep_ref[:128, at].astype(F32) + left_ref[:, at].astype(F32)).astype(BF)
        out_ref[k, 128:, :] = (keep_ref[128:, at].astype(F32) + right_ref[:, at].astype(F32)).astype(BF)


def sum_y(keep, left, right):
    return call(
        sum_y_kernel,
        jax.ShapeDtypeStruct((4, B, 512), BF),
        (keep, left, right),
        8,
        TOK * D,
        3 * MB,
        in_specs=[VM] * 3,
        out_specs=VM,
        name="sum_y",
    )


def sum_y4_kernel(in_ref, send_ref, keep_ref):
    zh = lax.axis_index("zh")

    def total(z):
        at = aligned(z * B, B)
        s = in_ref[0, :, at].astype(F32)
        for k in range(1, 4):
            s = s + in_ref[k, :, at].astype(F32)
        return s

    send_ref[...] = total(1 - zh).astype(BF)
    keep_ref[...] = total(zh)


def sum_y4(got):
    return call(
        sum_y4_kernel,
        (jax.ShapeDtypeStruct((B, B), BF), jax.ShapeDtypeStruct((B, B), F32)),
        (got,),
        6,
        TOK * D,
        2 * MB,
        in_specs=[VM],
        out_specs=(VM, VM),
        name="sum_y4",
    )


def last_kernel(main_ref, keep_ref, got_ref, gain_ref, gain_main_ref, out_ref, gain_out_ref):
    n = NY * NH * NC
    total = gain_ref[0]
    for i in range(1, NY * NC):
        total = total + gain_ref[i]
    gain_out_ref[...] = gain_main_ref[...] + total / n
    s = keep_ref[...] + got_ref[...].astype(F32)
    out_ref[...] = main_ref[...] + s.T / n


def last(main, keep, got, gain, gain_main):
    return call(
        last_kernel,
        (jax.ShapeDtypeStruct((B, B), F32), jax.ShapeDtypeStruct((1, B), F32)),
        (main, keep, got, gain, gain_main),
        4,
        B * B * 4,
        MB,
        in_specs=[VM] * 5,
        out_specs=(VM, VM),
        name="last",
    )


def gain_mix_kernel(own_ref, got_ref, out_ref):
    total = own_ref[...] + got_ref[...]
    for i in range(NY * NC):
        out_ref[i] = total


def gain_mix(own, got):
    return call(
        gain_mix_kernel,
        jax.ShapeDtypeStruct((NY * NC, 1, B), F32),
        (own, got),
        4,
        B,
        MB // 16,
        in_specs=[VM] * 2,
        out_specs=VM,
        name="gain_mix",
    )


def pairs(n, f):
    return [(i, f(i) % n) for i in range(n)]


def swap(v, axis, n, f):
    return lax.ppermute(v, axis, pairs(n, f))


def exchange(v, axis, **kw):
    return lax.all_to_all(v, axis, 0, 0, tiled=True, **kw)


def body(hidden, gain, weight, q_grad, q_main, gain_main):
    gain2 = gain.reshape(64, 128)
    part = partial(q_grad, weight, hidden, gain2)
    groups = [list(range(i * NG, (i + 1) * NG)) for i in range(NZ * NX // NG)]
    part = exchange(part, ("zl", "x"), axis_index_groups=groups)

    send, own, rinv = norm(hidden, gain2, q_grad)
    got = swap(send, "c", NC, lambda i: i ^ 1)
    left, right = product(sent_kernel, own, got, q_grad, 0, (128, 128), "sent")
    (keep,) = product(kept_kernel, own, got, q_grad, STEPS, (B,), "kept")
    left = swap(left, "y", NY, lambda i: i ^ 1)
    right = swap(right, "y", NY, lambda i: i + 1 if i % 2 else i - 1)

    send2, keep2 = sum_xz(part)
    got2 = swap(send2, "zl", NZ, lambda i: i ^ 2)

    four = sum_y(keep, left, right)
    four = exchange(four, "y", axis_index_groups=[[0, 2, 4, 6], [1, 3, 5, 7]])

    send3, keep3 = sum_z(keep2, got2, 2, 4)
    got3 = swap(send3, "zl", NZ, lambda i: i ^ 4)
    grad, own_gain = finish(keep3, got3, hidden, gain2, rinv)
    got_gain = swap(own_gain, "zh", NH, lambda i: i ^ 1)

    send_h, keep_h = sum_y4(four)
    got_h = swap(send_h, "zh", NH, lambda i: i ^ 1)
    all_gain = exchange(gain_mix(own_gain, got_gain), ("y", "c"))
    q_new, gain_new = last(q_main, keep_h, got_h, all_gain, gain_main.reshape(1, B))
    gain_new = gain_new.reshape(B)
    return grad, q_new, gain_new


def solution(mesh):
    fine = Mesh(mesh.devices.reshape(NY, NH, NC, NZ, NX), ("y", "zh", "c", "zl", "x"))
    dp, tp = ("y", "zh", "c"), ("zl", "x")
    in_specs = (P(dp, None), P(), P(None, tp), P(dp, tp), P(dp, tp), P(tp))
    out_specs = (P(dp, tp), P(dp, tp), P(tp))
    return jax.shard_map(body, mesh=fine, in_specs=in_specs, out_specs=out_specs, check_vma=False)
```

```python
import functools

import jax
import jax.numpy as jnp
from jax import lax
from jax.experimental import pallas as pl
from jax.experimental.pallas import tpu as pltpu
from jax.sharding import Mesh, PartitionSpec as P


BF = jnp.bfloat16
F32 = jnp.float32
NY, NH, NC, NZ, NX = 8, 2, 2, 8, 4
TOK = 128
D = 8192
B = 256
MB = 2**20
VM = pl.BlockSpec(memory_space=pltpu.VMEM)


def cost(flops, nbytes):
    return pl.CostEstimate(flops=flops, bytes_accessed=nbytes, transcendentals=0)


def params(mib):
    return pltpu.CompilerParams(vmem_limit_bytes=mib * MB if mib else None)


def call(kernel, out_shape, args, mib, flops, nbytes, **kw):
    return pl.pallas_call(
        kernel,
        out_shape=out_shape,
        compiler_params=params(mib),
        cost_estimate=cost(flops, nbytes),
        **kw,
    )(*args)


def aligned(start, size):
    return pl.ds(pl.multiple_of(start, size), size)


def two_rows(g_ref, block):
    at = lambda i: g_ref[pl.ds(2 * block + i, 1), :]
    return jnp.concatenate([at(0), at(1)], axis=1)


ROWS = 32


def norm_kernel(h_ref, g_ref, q_ref, send_ref, own_ref, rinv_ref, g32):
    par, core = lax.rem(lax.axis_index("y"), 2), lax.axis_index("c")
    g32[...] = g_ref[...].astype(F32)
    acc = jnp.zeros((ROWS, 128), F32)
    for j in range(D // 128):
        h = h_ref[:, j * 128 : (j + 1) * 128].astype(F32)
        acc = acc + h * h
    rinv = lax.rsqrt(jnp.sum(acc, axis=1, keepdims=True) / D + 1e-05)
    rinv_ref[...] = rinv
    for out, which in ((send_ref, 1 - core), (own_ref, core)):
        for j in range(16):
            o, k, zh = j // 8, (j // 2) % 4, j % 2
            y = 2 * k + (1 - par if o == 0 else par)
            block = y * 4 + zh * 2 + which
            h = h_ref[:, aligned(block * B, B)].astype(F32)
            out[:, j * B : (j + 1) * B] = (h * rinv * two_rows(g32, block)).astype(BF)
    send_ref[:, 16 * B :] = q_ref[...]


def norm(hidden, gain, q_grad):
    row = lambda n: pl.BlockSpec((ROWS, n), lambda i: (i, 0))
    return call(
        norm_kernel,
        (
            jax.ShapeDtypeStruct((TOK, 17 * B), BF),
            jax.ShapeDtypeStruct((TOK, 16 * B), BF),
            jax.ShapeDtypeStruct((TOK, 1), F32),
        ),
        (hidden, gain, q_grad),
        56,
        6 * TOK * D,
        4 * TOK * D,
        grid=(TOK // ROWS,),
        in_specs=[row(D), pl.BlockSpec((64, 128), lambda i: (0, 0)), row(B)],
        out_specs=(row(17 * B), row(16 * B), row(1)),
        scratch_shapes=[pltpu.VMEM((64, 128), F32)],
        name="norm",
    )


def eye():
    a = lax.broadcasted_iota(jnp.int32, (128, 128), 0)
    b = lax.broadcasted_iota(jnp.int32, (128, 128), 1)
    return a == b


def stat_rows(row):
    hi = row.astype(BF).astype(F32)
    both = jnp.concatenate([hi, row - hi], axis=1)
    first = lax.broadcasted_iota(jnp.int32, (8, 256), 0) == 0
    return jnp.where(first, jnp.broadcast_to(both, (8, 256)), 0.0).astype(BF)


def stat_of(block):
    both = jnp.sum(block.astype(F32), axis=0, keepdims=True)
    return both[:, :128] + both[:, 128:]


ZQ = NZ // 2
NG = 2 * NX
PIECE = ZQ * TOK + 8


def partial_kernel(q_ref, g_ref, w_hbm, h_hbm, out_hbm, w_ref, h_ref, out_ref, w_sem, h_sem, out_sem):
    wide = NX * B

    def w_copy(z):
        at = slice(z * wide, (z + 1) * wide)
        return pltpu.make_async_copy(w_hbm.at[at, :], w_ref.at[at, :], w_sem.at[z])

    def h_copy(z):
        at = slice(z * wide, (z + 1) * wide)
        return pltpu.make_async_copy(h_hbm.at[:, at], h_ref.at[:, at], h_sem.at[z])

    def out_copy(z, x):
        at = (z % 2 * NX + x, slice(z // 2 * TOK, (z // 2 + 1) * TOK))
        return pltpu.make_async_copy(out_ref.at[at], out_hbm.at[at], out_sem.at[z * NX + x])

    def stat_copy(d):
        at = (d, slice(ZQ * TOK, PIECE))
        return pltpu.make_async_copy(out_ref.at[at], out_hbm.at[at], out_sem.at[NZ * NX + d])

    for z in range(NZ):
        w_copy(z).start()
        h_copy(z).start()
    q = q_ref[...]
    g = g_ref[...].astype(F32)
    acc = jnp.zeros((TOK, 128), F32)
    for z in range(NZ):
        w_copy(z).wait()
        h_copy(z).wait()
        for x in range(NX):
            b = z * NX + x
            at = slice(b * B, (b + 1) * B)
            p = lax.dot_general(q, w_ref[at, :], (((1,), (1,)), ((), ())), preferred_element_type=F32)
            p = p.astype(BF)
            out_ref[z % 2 * NX + x, z // 2 * TOK : (z // 2 + 1) * TOK, :] = p
            t = p.astype(F32) * h_ref[:, at].astype(F32)
            acc = acc + t[:, :128] * g[2 * b : 2 * b + 1, :] + t[:, 128:] * g[2 * b + 1 : 2 * b + 2, :]
        if z > 0:
            for x in range(NX):
                out_copy(z - 1, x).start()
    s = jnp.sum(acc, axis=1, keepdims=True)
    rows = stat_rows(jnp.sum(jnp.where(eye(), s, 0.0), axis=0, keepdims=True))
    for d in range(NG):
        out_ref[d, ZQ * TOK :, :] = rows
    for x in range(NX):
        out_copy(NZ - 1, x).start()
    for d in range(NG):
        stat_copy(d).start()
    for z in range(NZ):
        for x in range(NX):
            out_copy(z, x).wait()
    for d in range(NG):
        stat_copy(d).wait()


HBM = pl.BlockSpec(memory_space=pltpu.HBM)


def partial(q_grad, weight, hidden, gain):
    return call(
        partial_kernel,
        jax.ShapeDtypeStruct((NG, PIECE, B), BF),
        (q_grad, gain, weight, hidden),
        None,
        2 * TOK * D * B,
        8 * MB,
        in_specs=[VM, VM, HBM, HBM],
        out_specs=HBM,
        scratch_shapes=[
            pltpu.VMEM((D, B), BF),
            pltpu.VMEM((TOK, D), BF),
            pltpu.VMEM((NG, PIECE, B), BF),
            pltpu.SemaphoreType.DMA((NZ,)),
            pltpu.SemaphoreType.DMA((NZ,)),
            pltpu.SemaphoreType.DMA((NZ * NX + NG,)),
        ],
        name="partial",
    )


def sum_xz_kernel(in_ref, send_ref, keep_ref):
    bit = lax.rem(lax.div(lax.axis_index("zl"), 2), 2)

    def total(at):
        s = in_ref[0, at, :].astype(F32)
        for d in range(1, NG):
            s = s + in_ref[d, at, :].astype(F32)
        return s

    rows = stat_rows(stat_of(total(slice(ZQ * TOK, PIECE))))
    for k in range(ZQ // 2):
        at = slice(k * TOK, (k + 1) * TOK)
        send_ref[at, :] = total(aligned((2 * k + 1 - bit) * TOK, TOK)).astype(BF)
        keep_ref[at, :] = total(aligned((2 * k + bit) * TOK, TOK))
    send_ref[ZQ // 2 * TOK :, :] = rows
    keep_ref[ZQ // 2 * TOK :, :] = rows.astype(F32)


def sum_xz(got):
    rows = ZQ // 2 * TOK + 8
    return call(
        sum_xz_kernel,
        (jax.ShapeDtypeStruct((rows, B), BF), jax.ShapeDtypeStruct((rows, B), F32)),
        (got,),
        12,
        TOK * D,
        4 * MB,
        in_specs=[VM],
        out_specs=(VM, VM),
        name="sum_xz",
    )


def sum_z_kernel(count, shift, keep_ref, got_ref, send_ref, out_ref):
    bit = lax.rem(lax.div(lax.axis_index("zl"), shift), 2)
    half = count // 2

    def total(at):
        return keep_ref[at, :] + got_ref[at, :].astype(F32)

    for k in range(half):
        at = slice(k * TOK, (k + 1) * TOK)
        send_ref[at, :] = total(aligned((2 * k + 1 - bit) * TOK, TOK)).astype(BF)
    rows = stat_rows(stat_of(total(slice(count * TOK, count * TOK + 8))))
    send_ref[half * TOK :, :] = rows
    for k in range(half):
        at = slice(k * TOK, (k + 1) * TOK)
        out_ref[at, :] = total(aligned((2 * k + bit) * TOK, TOK))
    out_ref[half * TOK :, :] = rows.astype(F32)


def sum_z(keep, got, count, shift):
    rows = count // 2 * TOK + 8
    return call(
        functools.partial(sum_z_kernel, count, shift),
        (jax.ShapeDtypeStruct((rows, B), BF), jax.ShapeDtypeStruct((rows, B), F32)),
        (keep, got),
        6,
        count * TOK * B,
        count * MB // 2,
        in_specs=[VM, VM],
        out_specs=(VM, VM),
        name=f"sum_z{shift}",
    )


def finish_kernel(keep_ref, got_ref, h_ref, g_ref, rinv_ref, out_ref, gain_ref, g32):
    own = lax.axis_index("zl") * NX + lax.axis_index("x")
    g32[...] = g_ref[...].astype(F32)
    grad = keep_ref[:TOK, :] + got_ref[:TOK, :].astype(F32)
    stat = stat_of(keep_ref[TOK:, :] + got_ref[TOK:, :].astype(F32))
    rinv = rinv_ref[...]
    stat = jnp.sum(jnp.where(eye(), stat, 0.0), axis=1, keepdims=True) * rinv / D
    xhat = h_ref[:, aligned(own * B, B)].astype(F32) * rinv
    gain_ref[...] = jnp.sum(grad * xhat, axis=0, keepdims=True)
    out_ref[...] = (rinv * (grad * two_rows(g32, own) - xhat * stat)).astype(BF)


def finish(keep, got, hidden, gain, rinv):
    return call(
        finish_kernel,
        (
            jax.ShapeDtypeStruct((TOK, B), BF),
            jax.ShapeDtypeStruct((1, B), F32),
        ),
        (keep, got, hidden, gain, rinv),
        10,
        TOK * B * 16,
        MB,
        in_specs=[VM] * 5,
        out_specs=(VM, VM),
        scratch_shapes=[pltpu.VMEM((64, 128), F32)],
        name="finish",
    )


STEPS = 4


def product_kernel(own_ref, got_ref, q_ref, gq_ref, left_ref, right_ref, keep_ref):
    i = pl.program_id(0)
    a = jnp.concatenate([own_ref[...], got_ref[...]], axis=0)
    q = jnp.concatenate([q_ref[...], gq_ref[...]], axis=0)
    p = lax.dot_general(q, a, (((0,), (0,)), ((), ())), preferred_element_type=F32).astype(BF)

    @pl.when(i < STEPS // 2)
    def _():
        left_ref[...] = p[:128, :]
        right_ref[...] = p[128:, :]

    @pl.when(i >= STEPS // 2)
    def _():
        keep_ref[...] = p


def product(own, got, q_grad):
    w = 16 * B // STEPS
    half = jax.ShapeDtypeStruct((128, 8 * B), BF)
    first = lambda i: (0, jnp.minimum(i, STEPS // 2 - 1))
    return call(
        product_kernel,
        (half, half, jax.ShapeDtypeStruct((B, 8 * B), BF)),
        (own, got, q_grad, got),
        16,
        2 * TOK * D * B,
        4 * MB,
        grid=(STEPS,),
        in_specs=[
            pl.BlockSpec((TOK, w), lambda i: (0, i)),
            pl.BlockSpec((TOK, w), lambda i: (0, i)),
            pl.BlockSpec((TOK, B), lambda i: (0, 0)),
            pl.BlockSpec((TOK, B), lambda i: (0, 16)),
        ],
        out_specs=(
            pl.BlockSpec((128, w), first),
            pl.BlockSpec((128, w), first),
            pl.BlockSpec((B, w), lambda i: (0, jnp.maximum(i - STEPS // 2, 0))),
        ),
        name="product",
    )


def sum_y_kernel(keep_ref, left_ref, right_ref, out_ref):
    for k in range(4):
        at = slice(k * 512, (k + 1) * 512)
        out_ref[k, :128, :] = (keep_ref[:128, at].astype(F32) + left_ref[:, at].astype(F32)).astype(BF)
        out_ref[k, 128:, :] = (keep_ref[128:, at].astype(F32) + right_ref[:, at].astype(F32)).astype(BF)


def sum_y(keep, left, right):
    return call(
        sum_y_kernel,
        jax.ShapeDtypeStruct((4, B, 512), BF),
        (keep, left, right),
        8,
        TOK * D,
        3 * MB,
        in_specs=[VM] * 3,
        out_specs=VM,
        name="sum_y",
    )


def sum_y4_kernel(in_ref, send_ref, keep_ref):
    zh = lax.axis_index("zh")

    def total(z):
        at = aligned(z * B, B)
        s = in_ref[0, :, at].astype(F32)
        for k in range(1, 4):
            s = s + in_ref[k, :, at].astype(F32)
        return s

    send_ref[...] = total(1 - zh).astype(BF)
    keep_ref[...] = total(zh)


def sum_y4(got):
    return call(
        sum_y4_kernel,
        (jax.ShapeDtypeStruct((B, B), BF), jax.ShapeDtypeStruct((B, B), F32)),
        (got,),
        6,
        TOK * D,
        2 * MB,
        in_specs=[VM],
        out_specs=(VM, VM),
        name="sum_y4",
    )


def last_kernel(main_ref, keep_ref, got_ref, gain_ref, gain_main_ref, out_ref, gain_out_ref):
    n = NY * NH * NC
    total = gain_ref[0]
    for i in range(1, NY * NC):
        total = total + gain_ref[i]
    gain_out_ref[...] = gain_main_ref[...] + total / n
    s = keep_ref[...] + got_ref[...].astype(F32)
    out_ref[...] = main_ref[...] + s.T / n


def last(main, keep, got, gain, gain_main):
    return call(
        last_kernel,
        (jax.ShapeDtypeStruct((B, B), F32), jax.ShapeDtypeStruct((1, B), F32)),
        (main, keep, got, gain, gain_main),
        4,
        B * B * 4,
        MB,
        in_specs=[VM] * 5,
        out_specs=(VM, VM),
        name="last",
    )


def gain_mix_kernel(own_ref, got_ref, out_ref):
    total = own_ref[...] + got_ref[...]
    for i in range(NY * NC):
        out_ref[i] = total


def gain_mix(own, got):
    return call(
        gain_mix_kernel,
        jax.ShapeDtypeStruct((NY * NC, 1, B), F32),
        (own, got),
        4,
        B,
        MB // 16,
        in_specs=[VM] * 2,
        out_specs=VM,
        name="gain_mix",
    )


def pairs(n, f):
    return [(i, f(i) % n) for i in range(n)]


def swap(v, axis, n, f):
    return lax.ppermute(v, axis, pairs(n, f))


def exchange(v, axis, **kw):
    return lax.all_to_all(v, axis, 0, 0, tiled=True, **kw)


def body(hidden, gain, weight, q_grad, q_main, gain_main):
    gain2 = gain.reshape(64, 128)
    part = partial(q_grad, weight, hidden, gain2)
    groups = [list(range(i * NG, (i + 1) * NG)) for i in range(NZ * NX // NG)]
    part = exchange(part, ("zl", "x"), axis_index_groups=groups)

    send, own, rinv = norm(hidden, gain2, q_grad)
    got = swap(send, "c", NC, lambda i: i ^ 1)
    left, right, keep = product(own, got, q_grad)
    left = swap(left, "y", NY, lambda i: i ^ 1)
    right = swap(right, "y", NY, lambda i: i + 1 if i % 2 else i - 1)

    send2, keep2 = sum_xz(part)
    got2 = swap(send2, "zl", NZ, lambda i: i ^ 2)

    four = sum_y(keep, left, right)
    four = exchange(four, "y", axis_index_groups=[[0, 2, 4, 6], [1, 3, 5, 7]])

    send3, keep3 = sum_z(keep2, got2, 2, 4)
    got3 = swap(send3, "zl", NZ, lambda i: i ^ 4)
    grad, own_gain = finish(keep3, got3, hidden, gain2, rinv)
    got_gain = swap(own_gain, "zh", NH, lambda i: i ^ 1)

    send_h, keep_h = sum_y4(four)
    got_h = swap(send_h, "zh", NH, lambda i: i ^ 1)
    all_gain = exchange(gain_mix(own_gain, got_gain), ("y", "c"))
    q_new, gain_new = last(q_main, keep_h, got_h, all_gain, gain_main.reshape(1, B))
    gain_new = gain_new.reshape(B)
    return grad, q_new, gain_new


def solution(mesh):
    fine = Mesh(mesh.devices.reshape(NY, NH, NC, NZ, NX), ("y", "zh", "c", "zl", "x"))
    dp, tp = ("y", "zh", "c"), ("zl", "x")
    in_specs = (P(dp, None), P(), P(None, tp), P(dp, tp), P(dp, tp), P(tp))
    out_specs = (P(dp, tp), P(dp, tp), P(tp))
    return jax.shard_map(body, mesh=fine, in_specs=in_specs, out_specs=out_specs, check_vma=False)
```
